128 devices in a mesh: grp: 4 (over x, y), tok: 16 (over z), mdl: 2 (over core).
Axes of the slice: x: 2, y: 2, z: 16, core: 2. Of those that a mesh axis runs over, the one named last changes fastest.
The devices are a block of a 8x8x16 slice.
Arguments:
- hidden: bfloat16 [4096, 4096], P(('grp', 'tok'), 'mdl'), parts along dimension 0, may hold values from -3 to 3
- queries: bfloat16 [4096, 16, 128], P(('grp', 'tok'), 'mdl'), parts along dimension 0, may hold values from -8 to 8
- cache: bfloat16 [64, 2048, 4, 2, 128], P(('grp', 'tok'), None, 'mdl'), parts along dimension 0, may hold values from -8 to 8
- cache_lengths: int32 [64], P(('grp', 'tok')), parts along dimension 0, may hold values from 128 to 2048, as said below
- wkv: bfloat16 [4096, 4, 2, 128], P('tok', 'mdl'), may hold values from -0.09375 to 0.09375
- wo: bfloat16 [16, 128, 4096], P('mdl', None, 'tok'), may hold values from -0.5 to 0.5
- attn_gain: bfloat16 [4096], replicated, may hold values from 0.5 to 1.5
- moe_gain: bfloat16 [4096], replicated, may hold values from 0.5 to 1.5
- w_gate: bfloat16 [32, 4096, 896], P(('tok', 'mdl')), may hold values from -0.09375 to 0.09375
- w_up: bfloat16 [32, 4096, 896], P(('tok', 'mdl')), may hold values from -0.09375 to 0.09375
- w_down: bfloat16 [32, 896, 4096], P(('tok', 'mdl')), may hold values from -0.0625 to 0.0625
- expert_ids: int32 [4096, 2], P(('grp', 'tok', 'mdl')), parts along dimension 0, may hold values from 0 to 3, all different within a row; in each aligned block of 32 rows (0 to 31, 32 to 63, ...) at most 18 rows name the same one
- gates: float32 [4096, 2], P(('grp', 'tok', 'mdl')), parts along dimension 0, may hold values from 0.1 to 1
Outputs:
- mixed: bfloat16 [4096, 4096], P(('grp', 'tok', 'mdl')), parts along dimension 0
- fresh_key_value: bfloat16 [4096, 4, 2, 128], P(('grp', 'tok'), 'mdl'), parts along dimension 0
The draws below stay inside these ranges and needn't reach their ends.
There are 4 independent parts, one for each index of `grp`. The reference program is written for one: setup_inputs(seed, part) draws one part's arguments, and reference() takes and returns one part's arrays. A program takes and returns all parts, laid end to end along the dimension named above; an argument that names none is the same for every part. Nothing has to cross between parts.
Inputs may be any that keep to these rules, and one draw needn't show every extreme that they name: `expert_ids`: each token names 2 different experts; in aligned blocks of 32 rows no expert is named by more than 18 rows, a bound that some block reaches. `cache_lengths`: some rollout holds exactly 2048 cached positions.
All inputs are finite; a program needn't handle non-finite values.
Results may differ from the reference program's by a relative error of at most 0.007.
Values may be sent and summed in bfloat16 or wider, within the bound.
No kernel may reach another device: no remote copies, remote signals or barrier semaphores. Data moves between devices by JAX's collectives and lax.ppermute only.
A program may use at most 128 MiB of HBM per device.

```python
import math
import jax
import jax.numpy as jnp
import numpy as np
from jax import lax

MODEL_DIM = 4096
HEAD_SIZE = 128
QUERY_HEADS = 16
KEY_VALUE_HEADS = 4
EXPERTS = 4
FF = 7168
TOPK = 2
NEW_TOKEN_SPAN = 64
CACHE_LIMIT = 2048
ROLLOUT_COUNT = 16
TOKEN_TOTAL = 1024
TOK_MOE = 32
CAP = 18
SLABS = 8
FS = 896
N_TOK = 16
N_MDL = 2


def draw_queries(key, part):
    array_shape = (TOKEN_TOTAL, QUERY_HEADS, HEAD_SIZE)
    return jnp.clip(jax.random.normal(jax.random.fold_in(key, 1), array_shape, jnp.float32) * 2.5, -7.5, 7.5).astype(jnp.bfloat16)


def draw_cache(key, part):
    array_shape = (ROLLOUT_COUNT, CACHE_LIMIT, KEY_VALUE_HEADS, 2, HEAD_SIZE)
    return jnp.clip(jax.random.normal(jax.random.fold_in(key, 2), array_shape, jnp.float32), -5.0, 5.0).astype(jnp.bfloat16)


def draw_cache_lengths(key, part):
    values = jax.random.randint(jax.random.fold_in(key, 3), (ROLLOUT_COUNT,), CACHE_LIMIT // 16, CACHE_LIMIT + 1)
    longest = jax.random.randint(jax.random.fold_in(key, 4), (), 0, ROLLOUT_COUNT)
    return jnp.where(jnp.arange(ROLLOUT_COUNT) == longest, CACHE_LIMIT, values).astype(jnp.int32)


def block_scale(stream_key, dims, split, smallest, top_value):
    level = 1.0
    for position, shards_of in split:
        steps = jax.random.uniform(jax.random.fold_in(jax.random.fold_in(stream_key, 6), position), (shards_of,), jnp.float32, smallest / len(split), top_value / len(split))
        level = level * jnp.repeat(jnp.exp(steps), dims[position] // shards_of).reshape((-1,) + (1,) * (len(dims) - 1 - position))
    return level


def routed_block(stream_key, own, number, rows, count, top, most, slope):
    ranking = jax.random.permutation(stream_key, count)
    crowded, usual = load_shares(count, rows * top, most, slope, True), load_shares(count, rows * top, most, slope, False)
    places = jnp.arange(count)

    def named(tallies, rotation):
        used = int((tallies > 0).sum())
        fixed = max(1, used // 4)
        shifted = fixed + (places - fixed + rotation * (used - fixed)) % max(1, count - fixed)
        return jnp.zeros((count,), jnp.int32).at[ranking[jnp.where(places < fixed, places, shifted)]].set(jnp.asarray(tallies, jnp.int32))

    tallies = jnp.where(number % 4 == 0, named(crowded, number // 4), named(usual, number - number // 4 - 1))
    mixed = jax.random.permutation(jax.random.fold_in(own, 3), count)
    source_of, receiver = mixed[0:count // 2 * 2:2], mixed[1:count // 2 * 2:2]
    room = jnp.minimum(tallies[source_of] - 1, most - tallies[receiver]) // 2
    room = jnp.where((source_of == ranking[0]) | (receiver == ranking[0]) | (tallies[receiver] == 0), 0, jnp.maximum(room, 0))
    shifted = jax.random.randint(jax.random.fold_in(own, 4), (count // 2,), 0, 1 << 20) % (room + 1)
    tallies = tallies.at[source_of].add(-shifted).at[receiver].add(shifted)
    items = jnp.searchsorted(jnp.cumsum(tallies), jnp.arange(rows * top), side="right").astype(jnp.int32)
    grid = items.reshape(top, rows).T
    grid = grid[jax.random.permutation(jax.random.fold_in(own, 1), rows)]
    rotation = jax.random.randint(jax.random.fold_in(own, 2), (rows, 1), 0, top)
    return jnp.take_along_axis(grid, (jnp.arange(top)[None, :] + rotation) % top, axis=1)


def load_shares(amount, total, reach, skew, full):
    weights = [(1 << 20) // math.isqrt(rank ** skew) + 1 for rank in range(1, amount + 1)]
    largest = reach if full else min(reach, max(-(-total // amount), total * weights[0] // sum(weights)))
    least = 1 if total - largest >= amount - 1 else 0
    holding, surplus = [largest] + [least] * (amount - 1), total - largest - least * (amount - 1)
    while surplus > 0:
        candidates = [i for i in range(1, amount) if holding[i] < largest] or [i for i in range(1, amount) if holding[i] < reach]
        whole, left = sum([weights[i] for i in candidates]), surplus
        for i in candidates:
            extra = min(reach - holding[i], max(1, left * weights[i] // whole), surplus)
            holding[i] = holding[i] + extra
            surplus = surplus - extra
    return np.array(holding)


def bell_draw(rng, shape, width, most, split=(), kind=jnp.bfloat16):
    drawn = width * jax.random.normal(rng, shape, jnp.float32)
    if split:
        drawn = drawn * block_scale(rng, shape, split, -0.22, 0.18)
    return jnp.clip(drawn, -most, most).astype(kind)


def setup_inputs(seed: int = 0, part: int = 0) -> dict:
    key_of = jax.random.split(jax.random.key(seed), 14)
    part_keys = jax.random.split(jax.random.fold_in(key_of[13], part), 14)
    hidden = bell_draw(part_keys[0], (TOKEN_TOTAL, MODEL_DIM), 0.5, 3.0, ((0, 16), (1, 2)))
    queries = draw_queries(jax.random.fold_in(jax.random.fold_in(key_of[13], part), 71), part)
    cache = draw_cache(jax.random.fold_in(jax.random.fold_in(key_of[13], part), 71), part)
    cache_lengths = draw_cache_lengths(jax.random.fold_in(jax.random.fold_in(key_of[13], part), 71), part)
    wkv = bell_draw(key_of[4], (MODEL_DIM, KEY_VALUE_HEADS, 2, HEAD_SIZE), MODEL_DIM ** -0.5, 0.09375, ((0, 16), (1, 2)))
    wo = bell_draw(key_of[5], (QUERY_HEADS, HEAD_SIZE, MODEL_DIM), HEAD_SIZE ** -0.5, 0.5, ((0, 2), (2, 16)))
    attn_gain = jnp.clip(1.0 + 0.1 * jax.random.normal(key_of[6], (MODEL_DIM,), jnp.float32), 0.5, 1.5).astype(jnp.bfloat16)
    moe_gain = jnp.clip(1.0 + 0.1 * jax.random.normal(key_of[7], (MODEL_DIM,), jnp.float32), 0.5, 1.5).astype(jnp.bfloat16)
    w_gate = bell_draw(key_of[8], (EXPERTS * SLABS, MODEL_DIM, FS), MODEL_DIM ** -0.5, 0.09375, ((0, 32),))
    w_up = bell_draw(key_of[9], (EXPERTS * SLABS, MODEL_DIM, FS), MODEL_DIM ** -0.5, 0.09375, ((0, 32),))
    w_down = bell_draw(key_of[10], (EXPERTS * SLABS, FS, MODEL_DIM), FF ** -0.5, 0.0625, ((0, 32),))
    expert_ids_keys = jax.random.split(jax.random.fold_in(part_keys[11], 1), TOKEN_TOTAL // TOK_MOE)
    expert_ids_turns = jax.random.permutation(jax.random.fold_in(part_keys[11], 3), TOKEN_TOTAL // TOK_MOE)
    expert_ids = jax.vmap(lambda own, number: routed_block(jax.random.fold_in(part_keys[11], 2), own, number, TOK_MOE, EXPERTS, TOPK, CAP, 2))(expert_ids_keys, expert_ids_turns).reshape((TOKEN_TOTAL, TOPK))
    gates = jnp.clip(0.1 + 0.9 * jax.random.uniform(part_keys[12], (TOKEN_TOTAL, TOPK), jnp.float32) ** block_scale(part_keys[12], (TOKEN_TOTAL, TOPK), ((0, 32),), -0.2, 0.2), 0.1, 1.0)
    return dict(hidden=hidden, queries=queries, cache=cache, cache_lengths=cache_lengths, wkv=wkv, wo=wo, attn_gain=attn_gain, moe_gain=moe_gain, w_gate=w_gate, w_up=w_up, w_down=w_down, expert_ids=expert_ids, gates=gates)


eps_norm = 1e-05
rope_base = 1000000.0
mask_fill = -1e+30

def rms_scale(values_in, gain):
    values = values_in.astype(jnp.float32)
    meansq = lax.optimization_barrier(jnp.mean(values * values, axis=-1, keepdims=True))
    return values * lax.rsqrt(meansq + eps_norm) * gain.astype(jnp.float32)

def rotate(key_rows, positions):
    half_dim = key_rows.shape[-1] // 2
    inverse = jnp.exp(jnp.arange(half_dim, dtype=jnp.float32) * (-2.0 * math.log(rope_base) / key_rows.shape[-1]))
    angle = positions.astype(jnp.float32)[:, None] * inverse[None, :]
    cosine = jnp.cos(angle)[:, None, :]
    sine_vals = jnp.sin(angle)[:, None, :]
    front_half = key_rows[..., :half_dim]
    back_half = key_rows[..., half_dim:]
    return jnp.concatenate([front_half * cosine - back_half * sine_vals, back_half * cosine + front_half * sine_vals], axis=-1)

def reference(hidden, queries, cache, cache_lengths, wkv, wo, attn_gain, moe_gain, w_gate, w_up, w_down, expert_ids, gates):
    normalized_input = rms_scale(hidden, attn_gain).astype(jnp.bfloat16)
    key_value_projection = jnp.dot(normalized_input, wkv.reshape(MODEL_DIM, KEY_VALUE_HEADS * 2 * HEAD_SIZE), preferred_element_type=jnp.float32).reshape(TOKEN_TOTAL, KEY_VALUE_HEADS, 2, HEAD_SIZE)
    positions = (cache_lengths[:, None] + jnp.arange(NEW_TOKEN_SPAN, dtype=jnp.int32)[None, :]).reshape(TOKEN_TOTAL).astype(jnp.int32)
    fresh_key_value = jnp.stack([rotate(key_value_projection[:, :, 0], positions), key_value_projection[:, :, 1]], axis=2).astype(jnp.bfloat16)
    head_group = QUERY_HEADS // KEY_VALUE_HEADS
    scale_factor = 1.0 / math.sqrt(HEAD_SIZE)
    query_all = queries.reshape(ROLLOUT_COUNT, NEW_TOKEN_SPAN, QUERY_HEADS, HEAD_SIZE)
    fresh_all_rows = fresh_key_value.reshape(ROLLOUT_COUNT, NEW_TOKEN_SPAN, KEY_VALUE_HEADS, 2, HEAD_SIZE)

    def one_rollout(packed):
        query_roll, cache_roll, new_roll, length = packed
        token_of_row = jnp.arange(NEW_TOKEN_SPAN * head_group) // head_group
        column = jnp.arange(CACHE_LIMIT + NEW_TOKEN_SPAN)
        allowed = jnp.where(column[None, :] < CACHE_LIMIT, column[None, :] < length, column[None, :] - CACHE_LIMIT <= token_of_row[:, None])
        outputs = []
        for head_index in range(KEY_VALUE_HEADS):
            query_rows = query_roll[:, head_index * head_group:(head_index + 1) * head_group].reshape(NEW_TOKEN_SPAN * head_group, HEAD_SIZE)
            key_rows = jnp.concatenate([cache_roll[:, head_index, 0], new_roll[:, head_index, 0]], axis=0)
            value_rows = jnp.concatenate([cache_roll[:, head_index, 1], new_roll[:, head_index, 1]], axis=0)
            scores = lax.dot_general(query_rows, key_rows, (((1,), (1,)), ((), ())), preferred_element_type=jnp.float32) * scale_factor
            scores = jnp.where(allowed, scores, mask_fill)
            row_max = lax.optimization_barrier(jnp.max(scores, axis=1, keepdims=True))
            weights = jnp.where(allowed, jnp.exp(scores - row_max), 0.0)
            probs = (weights / lax.optimization_barrier(jnp.sum(weights, axis=1, keepdims=True))).astype(jnp.bfloat16)
            attended = jnp.dot(probs, value_rows, preferred_element_type=jnp.float32).astype(jnp.bfloat16)
            outputs.append(attended.reshape(NEW_TOKEN_SPAN, head_group * HEAD_SIZE))
        return jnp.concatenate(outputs, axis=1)
    heads_out = lax.map(one_rollout, (query_all, cache, fresh_all_rows, cache_lengths)).reshape(TOKEN_TOTAL, QUERY_HEADS * HEAD_SIZE)
    attn_out = jnp.dot(heads_out, wo.reshape(QUERY_HEADS * HEAD_SIZE, MODEL_DIM), preferred_element_type=jnp.float32)
    resid = hidden.astype(jnp.float32) + attn_out
    moe_in = rms_scale(resid, moe_gain).astype(jnp.bfloat16)
    limit = N_TOK * N_MDL * CAP
    moe_out = jnp.zeros((TOKEN_TOTAL, MODEL_DIM), jnp.float32)
    for expert_idx in range(EXPERTS):
        match = expert_ids == expert_idx
        routed = jnp.any(match, axis=1)
        weight = lax.optimization_barrier(jnp.sum(jnp.where(match, gates, 0.0), axis=1)).astype(jnp.float32)
        order = jnp.argsort(jnp.where(routed, 0, 1).astype(jnp.int32), stable=True)[:limit].astype(jnp.int32)
        rows_in = moe_in[order]

        def slab_step(total, slab_idx):
            row_idx = expert_idx * SLABS + slab_idx
            gate_w = lax.dynamic_index_in_dim(w_gate, row_idx, 0, keepdims=False)
            up_w = lax.dynamic_index_in_dim(w_up, row_idx, 0, keepdims=False)
            down_w = lax.dynamic_index_in_dim(w_down, row_idx, 0, keepdims=False)
            gate_val = jnp.dot(rows_in, gate_w, preferred_element_type=jnp.float32)
            up_val = jnp.dot(rows_in, up_w, preferred_element_type=jnp.float32)
            slab_hidden = (jax.nn.silu(gate_val) * up_val).astype(jnp.bfloat16)
            slab_out = jnp.dot(slab_hidden, down_w, preferred_element_type=jnp.float32).astype(jnp.bfloat16)
            return (total + slab_out.astype(jnp.float32), None)
        total, unused = lax.scan(slab_step, jnp.zeros((limit, MODEL_DIM), jnp.float32), jnp.arange(SLABS, dtype=jnp.int32))
        moe_out = moe_out.at[order].add(weight[order][:, None] * total)
    mixed = (resid + moe_out).astype(jnp.bfloat16)
    return (mixed, fresh_key_value)
```

```python
import functools
import math

import jax
import jax.numpy as jnp
from jax import lax
from jax.experimental import pallas as pl
from jax.experimental.pallas import tpu as pltpu
from jax.sharding import PartitionSpec as P

EXPERTS = 4
TOPK = 2

eps_norm = 1e-05
rope_base = 1000000.0
mask_fill = -1e30


INTERPRET = False


def shift(x, step):
    size = lax.axis_size("tok")
    return lax.ppermute(x, "tok", [(i, (i + step) % size) for i in range(size)])


def swap(x):
    return lax.ppermute(x, "mdl", [(0, 1), (1, 0)])


def ring_gather(parts):
    size = lax.axis_size("tok")
    here = lax.axis_index("tok")
    yield here, parts
    up, down = list(parts), list(parts)
    for step in range(1, size // 2 + 1):
        up = [shift(p, 1) for p in up]
        last = step == size // 2
        if not last:
            down = [shift(p, -1) for p in down]
        yield (here - step) % size, up
        if not last:
            yield (here + step) % size, down


def ring_scatter_sum(pick):
    size = lax.axis_size("tok")
    here = lax.axis_index("tok")
    half = size // 2

    def joined(arrived, device):
        return [(a.astype(jnp.float32) + b.astype(jnp.float32)) for a, b in zip(arrived, pick(device))]

    up = pick((here + half) % size)
    down = pick((here - half + 1) % size)
    for step in range(1, half + 1):
        up = [shift(p, 1) for p in up]
        if step < half:
            up = [p.astype(jnp.bfloat16) for p in joined(up, (here + half - step) % size)]
            down = [shift(p, -1) for p in down]
            if step < half - 1:
                down = [p.astype(jnp.bfloat16) for p in joined(down, (here - half + 1 + step) % size)]
    own = pick(here)
    return [u.astype(jnp.float32) + d.astype(jnp.float32) + o.astype(jnp.float32) for u, d, o in zip(up, down, own)]


def rms_scale(values_in, gain):
    values = values_in.astype(jnp.float32)
    meansq = jnp.mean(values * values, axis=-1, keepdims=True)
    return values * lax.rsqrt(meansq + eps_norm) * gain.astype(jnp.float32)


def rotate(key_rows, positions):
    half_dim = key_rows.shape[-1] // 2
    inverse = jnp.exp(
        jnp.arange(half_dim, dtype=jnp.float32) * (-2.0 * math.log(rope_base) / key_rows.shape[-1])
    )
    angle = positions.astype(jnp.float32)[:, None] * inverse[None, :]
    cosine = jnp.cos(angle)[:, None, :]
    sine_vals = jnp.sin(angle)[:, None, :]
    front_half = key_rows[..., :half_dim]
    back_half = key_rows[..., half_dim:]
    return jnp.concatenate(
        [front_half * cosine - back_half * sine_vals, back_half * cosine + front_half * sine_vals],
        axis=-1,
    )


def expert_kernel(k_steps, x_ref, pick_ref, spread_ref, weight_ref, gain_ref, g0, u0, g1, u1, d0, d1, out_ref, xs, ss, ga, ua, hid):
    step = pl.program_id(0)
    width = xs.shape[1] // k_steps
    block = x_ref.shape[2]

    def dot(a, b):
        return jnp.dot(a, b, preferred_element_type=jnp.float32)

    def gate_up(k, gate_w, up_w, col):
        tile = xs[:, pl.ds(pl.multiple_of(k * width, width), width)]
        g = dot(tile, gate_w[0])
        u = dot(tile, up_w[0])

        @pl.when(k == 0)
        def _():
            ga[...] = g
            ua[...] = u

        @pl.when(k > 0)
        def _():
            ga[...] += g
            ua[...] += u

        @pl.when(k == k_steps - 1)
        def _():
            scale = lax.rsqrt(ss[:, :1] * (1.0 / xs.shape[1]) + eps_norm)
            gv = ga[...] * scale
            uv = ua[...] * scale
            hid[:, col : col + ga.shape[1]] = (gv / (1.0 + jnp.exp(-gv)) * uv).astype(jnp.bfloat16)

    @pl.when(step < k_steps)
    def _():
        total = jnp.zeros((xs.shape[0], 1), jnp.float32)
        for j in range(width // block):
            rows = dot(pick_ref[...], x_ref[step * (width // block) + j])
            total += jnp.sum(rows * rows, axis=1, keepdims=True)
            start = pl.multiple_of(step * width + j * block, block)
            xs[:, pl.ds(start, block)] = (rows * gain_ref[:, pl.ds(start, block)]).astype(jnp.bfloat16)

        @pl.when(step == 0)
        def _():
            ss[...] = jnp.broadcast_to(total, ss.shape)

        @pl.when(step > 0)
        def _():
            ss[...] += jnp.broadcast_to(total, ss.shape)

        gate_up(step, g0, u0, 0)

    @pl.when((step >= k_steps) & (step < 2 * k_steps))
    def _():
        gate_up(step - k_steps, g1, u1, ga.shape[1])

    @pl.when(step >= 2 * k_steps)
    def _():
        ff = ga.shape[1]
        rows = dot(hid[:, :ff], d0[0]) + dot(hid[:, ff:], d1[0])
        out_ref[...] = (dot(spread_ref[...], rows.astype(jnp.bfloat16)) * weight_ref[...]).astype(jnp.bfloat16)


def expert_rows(x, pick, spread, weight, gain, gates0, ups0, gates1, ups1, downs0, downs1):
    blocks, tokens, block = x.shape
    model = blocks * block
    ff = gates0.shape[2]
    rows = pick.shape[0]
    k_steps = 4
    width = model // k_steps
    whole = lambda shape: pl.BlockSpec(shape, lambda i: (0,) * len(shape))
    first = pl.BlockSpec((1, width, ff), lambda i: (0, jnp.minimum(i, k_steps - 1), 0))
    second = pl.BlockSpec((1, width, ff), lambda i: (0, jnp.clip(i - k_steps, 0, k_steps - 1), 0))
    third = pl.BlockSpec((1, ff, width), lambda i: (0, 0, jnp.maximum(i - 2 * k_steps, 0)))
    return pl.pallas_call(
        functools.partial(expert_kernel, k_steps),
        grid=(3 * k_steps,),
        in_specs=[
            whole(x.shape),
            whole(pick.shape),
            whole(spread.shape),
            whole(weight.shape),
            whole(gain.shape),
            first,
            first,
            second,
            second,
            third,
            third,
        ],
        out_specs=pl.BlockSpec((tokens, width), lambda i: (0, jnp.maximum(i - 2 * k_steps, 0))),
        out_shape=jax.ShapeDtypeStruct((tokens, model), jnp.bfloat16),
        scratch_shapes=[
            pltpu.VMEM((rows, model), jnp.bfloat16),
            pltpu.VMEM((rows, 128), jnp.float32),
            pltpu.VMEM((rows, ff), jnp.float32),
            pltpu.VMEM((rows, ff), jnp.float32),
            pltpu.VMEM((rows, 2 * ff), jnp.bfloat16),
        ],
        compiler_params=pltpu.CompilerParams(
            dimension_semantics=("arbitrary",), vmem_limit_bytes=48 * 1024 * 1024
        ),
        cost_estimate=pl.CostEstimate(
            flops=12 * rows * model * ff, bytes_accessed=12 * model * ff, transcendentals=2 * rows * ff
        ),
        interpret=INTERPRET,
        name="experts",
    )(x, pick, spread, weight, gain, gates0, ups0, gates1, ups1, downs0, downs1)


def shards(
    hidden,
    queries,
    cache,
    cache_lengths,
    wkv,
    wo,
    attn_gain,
    moe_gain,
    w_gate,
    w_up,
    w_down,
    expert_ids,
    gates,
):
    size = lax.axis_size("tok")
    here = lax.axis_index("tok")
    core = lax.axis_index("mdl")
    cores = lax.axis_size("mdl")
    bf16, f32 = jnp.bfloat16, jnp.float32

    other_hidden = swap(hidden)
    low = jnp.where(core == 0, hidden, other_hidden)
    high = jnp.where(core == 0, other_hidden, hidden)
    full_rows = jnp.concatenate([low, high], axis=1)
    span_len, model = full_rows.shape
    core_rows = span_len // cores
    kv_heads, head_dim = wkv.shape[1], wkv.shape[3]
    block = model // size

    normed = rms_scale(full_rows, attn_gain).astype(bf16)
    by_block = jnp.moveaxis(normed.reshape(span_len, size, block), 1, 0)
    own_kv = wkv.reshape(wkv.shape[0], -1)
    half = own_kv.shape[0] // 2
    kv = jnp.zeros((span_len, own_kv.shape[1]), f32)
    for source, (top, bottom) in ring_gather([own_kv[:half], own_kv[half:]]):
        part = lax.dynamic_index_in_dim(by_block, source, 0, keepdims=False)
        kv = kv + jnp.dot(part[:, :half], top, preferred_element_type=f32)
        kv = kv + jnp.dot(part[:, half:], bottom, preferred_element_type=f32)
    kv = kv.reshape(span_len, kv_heads, 2, head_dim)

    other_gate, other_up, other_down = swap(w_gate), swap(w_up), swap(w_down)
    own_wo = wo.reshape(-1, wo.shape[2])
    other_wo = swap(own_wo)
    full_wo = jnp.concatenate(
        [jnp.where(core == 0, own_wo, other_wo), jnp.where(core == 0, other_wo, own_wo)], axis=0
    )
    own_rows = lax.dynamic_slice_in_dim(full_rows, core * core_rows, core_rows, 0)
    hidden_cols = lax.all_to_all(
        jnp.moveaxis(own_rows.reshape(core_rows, size, block), 1, 0), "tok", 0, 0, tiled=True
    )
    matches = expert_ids[:, :, None] == jnp.arange(EXPERTS)[None, None, :]
    route = jnp.sum(jnp.where(matches, gates[:, :, None], 0.0), axis=1)
    weight = lax.all_to_all(
        jnp.repeat(route.T, size // EXPERTS, axis=0), "tok", 0, 0, tiled=True
    )
    chosen = (weight > 0).astype(jnp.int32)
    rank = jnp.cumsum(chosen, axis=1) - chosen
    capacity = core_rows * TOPK * 9 // (8 * EXPERTS)
    slot = jnp.where(chosen > 0, rank + jnp.arange(size)[:, None] * capacity, -1).reshape(1, -1)
    pick = (jnp.arange(size * capacity)[:, None] == slot).astype(bf16)
    spread = (slot.reshape(-1, 1) == jnp.arange(size * capacity)[None, :]).astype(bf16)

    length = cache_lengths[0]
    head_group = queries.shape[1] // kv_heads
    scale_factor = 1.0 / math.sqrt(head_dim)
    rows = jnp.transpose(
        queries.reshape(span_len, kv_heads, head_group, head_dim), (1, 0, 2, 3)
    ).reshape(kv_heads, span_len * head_group, head_dim)
    old_allowed = (jnp.arange(cache.shape[1]) < length)[None, None, :]
    keys = jnp.stack([cache[0, :, h, 0] for h in range(kv_heads)])
    values = jnp.stack([cache[0, :, h, 1] for h in range(kv_heads)])
    scores = jnp.einsum("hqd,hkd->hqk", rows, keys, preferred_element_type=f32) * scale_factor
    scores = jnp.where(old_allowed, scores, mask_fill)
    old_max = jnp.max(scores, axis=2, keepdims=True)
    old_probs = jnp.where(old_allowed, jnp.exp(scores - old_max), 0.0)
    old_sum = jnp.sum(old_probs, axis=2, keepdims=True)
    old_total = jnp.einsum("hqk,hkd->hqd", old_probs.astype(bf16), values, preferred_element_type=f32)

    positions = length + jnp.arange(span_len, dtype=jnp.int32)
    fresh_key_value = jnp.stack([rotate(kv[:, :, 0], positions), kv[:, :, 1]], axis=2).astype(bf16)
    new_keys = jnp.transpose(fresh_key_value[:, :, 0], (1, 0, 2))
    new_values = jnp.transpose(fresh_key_value[:, :, 1], (1, 0, 2))
    token_of_row = jnp.arange(span_len * head_group) // head_group
    new_allowed = (jnp.arange(span_len)[None, :] <= token_of_row[:, None])[None]
    new_scores = jnp.einsum("hqd,hkd->hqk", rows, new_keys, preferred_element_type=f32) * scale_factor
    new_scores = jnp.where(new_allowed, new_scores, mask_fill)
    row_max = jnp.maximum(old_max, jnp.max(new_scores, axis=2, keepdims=True))
    new_probs = jnp.where(new_allowed, jnp.exp(new_scores - row_max), 0.0)
    decay = jnp.exp(old_max - row_max)
    row_sum = old_sum * decay + jnp.sum(new_probs, axis=2, keepdims=True)
    attended = old_total * decay + jnp.einsum(
        "hqk,hkd->hqd", new_probs.astype(bf16), new_values, preferred_element_type=f32
    )
    attended = (attended / row_sum).astype(bf16)
    heads_out = jnp.transpose(
        attended.reshape(kv_heads, span_len, head_group, head_dim), (1, 0, 2, 3)
    ).reshape(cores, core_rows, -1)

    own_heads = lax.all_to_all(heads_out, "mdl", 0, 0, tiled=True)
    own_heads = jnp.moveaxis(own_heads, 0, 1).reshape(core_rows, -1)
    all_heads = jnp.zeros((size, *own_heads.shape), bf16)
    for source, (piece,) in ring_gather([own_heads]):
        all_heads = lax.dynamic_update_index_in_dim(all_heads, piece, source, 0)
    attn_cols = jnp.dot(
        all_heads.reshape(size * core_rows, -1), full_wo, preferred_element_type=f32
    )
    resid_cols = (hidden_cols.reshape(size * core_rows, block).astype(f32) + attn_cols).astype(bf16)

    middle = resid_cols.shape[0] // 2
    resid_all = jnp.zeros((size, *resid_cols.shape), bf16)
    for source, (top, bottom) in ring_gather([resid_cols[:middle], resid_cols[middle:]]):
        resid_all = lax.dynamic_update_slice(resid_all, top[None], (source, 0, 0))
        resid_all = lax.dynamic_update_slice(resid_all, bottom[None], (source, middle, 0))

    partial = expert_rows(
        resid_all,
        pick,
        spread,
        weight.reshape(-1, 1),
        moe_gain.astype(f32).reshape(1, -1),
        w_gate,
        w_up,
        other_gate,
        other_up,
        w_down,
        other_down,
    ).reshape(size, core_rows, model)

    def pieces(device):
        mine = lax.dynamic_index_in_dim(partial, device, 0, keepdims=False)
        return [mine[:, : model // 2], mine[:, model // 2 :]]

    moe_out = jnp.concatenate(ring_scatter_sum(pieces), axis=1)
    own_resid = lax.dynamic_slice_in_dim(resid_all, here * core_rows, core_rows, 1)
    own_resid = jnp.moveaxis(own_resid, 0, 1).reshape(core_rows, model).astype(f32)
    mixed = (own_resid + moe_out).astype(bf16)
    return (mixed, fresh_key_value)


def solution(mesh):
    in_specs = (
        P(("grp", "tok"), "mdl"),
        P(("grp", "tok"), "mdl", None),
        P(("grp", "tok"), None, "mdl", None, None),
        P(("grp", "tok")),
        P("tok", "mdl", None, None),
        P("mdl", None, "tok"),
        P(),
        P(),
        P(("tok", "mdl"), None, None),
        P(("tok", "mdl"), None, None),
        P(("tok", "mdl"), None, None),
        P(("grp", "tok", "mdl"), None),
        P(("grp", "tok", "mdl"), None),
    )
    out_specs = (P(("grp", "tok", "mdl"), None), P(("grp", "tok"), "mdl", None, None))
    return jax.shard_map(shards, mesh=mesh, in_specs=in_specs, out_specs=out_specs, check_vma=False)
```

```python
import functools
import math

import jax
import jax.numpy as jnp
from jax import lax
from jax.experimental import pallas as pl
from jax.experimental.pallas import tpu as pltpu
from jax.sharding import PartitionSpec as P

EXPERTS = 4
TOPK = 2

eps_norm = 1e-05
rope_base = 1000000.0
mask_fill = -1e30


INTERPRET = False


def shift(x, step):
    size = lax.axis_size("tok")
    return lax.ppermute(x, "tok", [(i, (i + step) % size) for i in range(size)])


def swap(x):
    return lax.ppermute(x, "mdl", [(0, 1), (1, 0)])


def ring_gather(parts):
    size = lax.axis_size("tok")
    here = lax.axis_index("tok")
    yield here, parts
    up, down = list(parts), list(parts)
    for step in range(1, size // 2 + 1):
        up = [shift(p, 1) for p in up]
        last = step == size // 2
        if not last:
            down = [shift(p, -1) for p in down]
        yield (here - step) % size, up
        if not last:
            yield (here + step) % size, down


def ring_scatter_sum(pick):
    size = lax.axis_size("tok")
    here = lax.axis_index("tok")
    half = size // 2

    def joined(arrived, device):
        return [(a.astype(jnp.float32) + b.astype(jnp.float32)) for a, b in zip(arrived, pick(device))]

    up = pick((here + half) % size)
    down = pick((here - half + 1) % size)
    for step in range(1, half + 1):
        up = [shift(p, 1) for p in up]
        if step < half:
            up = [p.astype(jnp.bfloat16) for p in joined(up, (here + half - step) % size)]
            down = [shift(p, -1) for p in down]
            if step < half - 1:
                down = [p.astype(jnp.bfloat16) for p in joined(down, (here - half + 1 + step) % size)]
    own = pick(here)
    return [u.astype(jnp.float32) + d.astype(jnp.float32) + o.astype(jnp.float32) for u, d, o in zip(up, down, own)]


def rms_scale(values_in, gain):
    values = values_in.astype(jnp.float32)
    meansq = jnp.mean(values * values, axis=-1, keepdims=True)
    return values * lax.rsqrt(meansq + eps_norm) * gain.astype(jnp.float32)


def dot(a, b):
    return jnp.dot(a, b, preferred_element_type=jnp.float32)


def score(a, b):
    return lax.dot_general(a, b, (((1,), (1,)), ((), ())), preferred_element_type=jnp.float32)


VMEM = pl.BlockSpec(memory_space=pltpu.VMEM)
SMEM = pl.BlockSpec(memory_space=pltpu.SMEM)
ANY = pl.BlockSpec(memory_space=pl.ANY)


def cache_kernel(scale, length_ref, q_ref, k_ref, v_ref, total_ref, max_ref, sum_ref, s_ref):
    length = length_ref[0]
    block = 512
    steps = k_ref.shape[1] // block
    q = q_ref[0]
    top = None
    for i in range(steps):
        s = score(q, k_ref[0, i * block : (i + 1) * block]) * scale
        column = i * block + lax.broadcasted_iota(jnp.int32, s.shape, 1)
        s = jnp.where(column < length, s, mask_fill)
        s_ref[:, i * block : (i + 1) * block] = s
        high = jnp.max(s, axis=1, keepdims=True)
        top = high if top is None else jnp.maximum(top, high)
    row_sum = jnp.zeros_like(top)
    total = jnp.zeros(total_ref.shape[1:], jnp.float32)
    for i in range(steps):
        s = s_ref[:, i * block : (i + 1) * block]
        column = i * block + lax.broadcasted_iota(jnp.int32, s.shape, 1)
        p = jnp.where(column < length, jnp.exp(s - top), 0.0)
        row_sum += jnp.sum(p, axis=1, keepdims=True)
        total += dot(p.astype(jnp.bfloat16), v_ref[0, i * block : (i + 1) * block])
    total_ref[0] = total
    max_ref[0] = jnp.broadcast_to(top, total.shape)
    sum_ref[0] = jnp.broadcast_to(row_sum, total.shape)


def cache_attention(length, rows, keys, values, scale):
    heads, count, dim = rows.shape
    per_head = lambda n: pl.BlockSpec((1, n, dim), lambda i: (i, 0, 0))
    out = jax.ShapeDtypeStruct((heads, count, dim), jnp.float32)
    return pl.pallas_call(
        functools.partial(cache_kernel, scale),
        grid=(heads,),
        in_specs=[SMEM, per_head(count), per_head(keys.shape[1]), per_head(keys.shape[1])],
        out_specs=[per_head(count)] * 3,
        out_shape=[out] * 3,
        scratch_shapes=[pltpu.VMEM((count, keys.shape[1]), jnp.float32)],
        compiler_params=pltpu.CompilerParams(
            dimension_semantics=("arbitrary",), vmem_limit_bytes=16 * 1024 * 1024
        ),
        cost_estimate=pl.CostEstimate(
            flops=4 * heads * count * dim * keys.shape[1],
            bytes_accessed=4 * keys.size,
            transcendentals=heads * count * keys.shape[1],
        ),
        interpret=INTERPRET,
        name="cache_attention",
    )(length, rows, keys, values)


def fresh_kernel(scale, order, *refs):
    parts = refs[: 2 * len(order)]
    n_ref, cos_ref, sin_ref, q_ref, total_ref, max_ref, sum_ref, heads_ref, fresh_ref = refs[2 * len(order) :]
    half = n_ref.shape[2] // 2
    span = n_ref.shape[1]
    kv = None
    for i, at in enumerate(order):
        more = dot(n_ref[at, :, :half], parts[2 * i][...]) + dot(n_ref[at, :, half:], parts[2 * i + 1][...])
        kv = more if kv is None else kv + more
    heads, count, dim = q_ref.shape
    group = count // span
    for h in range(heads):
        k = kv[:, 2 * h * dim : (2 * h + 1) * dim]
        v = kv[:, (2 * h + 1) * dim : (2 * h + 2) * dim].astype(jnp.bfloat16)
        k = (k * cos_ref[...] + pltpu.roll(k, dim // 2, 1) * sin_ref[...]).astype(jnp.bfloat16)
        fresh_ref[:, 2 * h * dim : (2 * h + 1) * dim] = k
        fresh_ref[:, (2 * h + 1) * dim : (2 * h + 2) * dim] = v
        s = score(q_ref[h], k) * scale
        token = lax.broadcasted_iota(jnp.int32, s.shape, 0) % span
        allowed = lax.broadcasted_iota(jnp.int32, s.shape, 1) <= token
        s = jnp.where(allowed, s, mask_fill)
        old_max = max_ref[h][:, :1]
        top = jnp.maximum(old_max, jnp.max(s, axis=1, keepdims=True))
        p = jnp.where(allowed, jnp.exp(s - top), 0.0)
        decay = jnp.exp(old_max - top)
        row_sum = sum_ref[h][:, :1] * decay + jnp.sum(p, axis=1, keepdims=True)
        out = (total_ref[h] * decay + dot(p.astype(jnp.bfloat16), v)) / row_sum
        for g in range(group):
            col = (h * group + g) * dim
            heads_ref[:, col : col + dim] = out[g * span : (g + 1) * span].astype(jnp.bfloat16)


def fresh_attention(parts, order, n_rot, cosine, sine, rows, old, scale):
    span = n_rot.shape[1]
    heads, count, dim = rows.shape
    return pl.pallas_call(
        functools.partial(fresh_kernel, scale, order),
        in_specs=[VMEM] * (len(parts) + 7),
        out_specs=[VMEM, VMEM],
        out_shape=[
            jax.ShapeDtypeStruct((span, heads * (count // span) * dim), jnp.bfloat16),
            jax.ShapeDtypeStruct((span, heads * 2 * dim), jnp.bfloat16),
        ],
        compiler_params=pltpu.CompilerParams(vmem_limit_bytes=24 * 1024 * 1024),
        interpret=INTERPRET,
        name="fresh_attention",
    )(*parts, n_rot, cosine, sine, rows, *old)


def output_kernel(places_ref, h0, h1, h2, h3a, h3b, c0, c1, c2, c3, *refs):
    weights = refs[:8]
    left_ref, right_ref, all_ref = refs[8:]
    n = h0.shape[0]
    all_ref[0:n] = h0[...]
    all_ref[n : 2 * n] = h1[...]
    all_ref[2 * n : 3 * n] = h2[...]
    all_ref[3 * n : 3 * n + n // 2] = h3a[...]
    all_ref[3 * n + n // 2 :] = h3b[...]
    half = all_ref.shape[1] // 2
    mine, other = all_ref[:, :half], all_ref[:, half:]
    block = c0.shape[2]
    for j in range(4):
        out = dot(mine, weights[j][...]) + dot(other, weights[4 + j][...])
        target = left_ref if j < 2 else right_ref
        for g, c in enumerate((c0, c1, c2, c3)):
            row = pl.multiple_of(places_ref[g] * n, n)
            value = out[g * n : (g + 1) * n] + c[j].astype(jnp.float32)
            target[pl.ds(row, n), (j % 2) * block : (j % 2 + 1) * block] = value.astype(jnp.bfloat16)


def output_rows(places, heads, cols, weights):
    n, width = heads[0].shape
    block = cols[0].shape[2]
    out = jax.ShapeDtypeStruct((4 * n, 2 * block), jnp.bfloat16)
    return pl.pallas_call(
        output_kernel,
        in_specs=[SMEM] + [VMEM] * 17,
        out_specs=[VMEM, VMEM],
        out_shape=[out, out],
        scratch_shapes=[pltpu.VMEM((4 * n, width), jnp.bfloat16)],
        compiler_params=pltpu.CompilerParams(vmem_limit_bytes=24 * 1024 * 1024),
        interpret=INTERPRET,
        name="output_rows",
    )(places, *heads, *cols, *weights)


def expert_kernel(sources, k_steps, ahead, src_ref, *refs):
    parts = refs[: 2 * sources]
    (pick_ref, spread_ref, weight_ref, gain_ref, g0, u0, g1, u1, d0, d1, out_ref, own_ref,
     x, wbuf, dbuf, wsem, xsem, xs, ga, ua, hid) = refs[2 * sources :]
    model = x.shape[1]
    ff = ga.shape[1]
    width = model // k_steps
    group = parts[0].shape[0]
    block = parts[0].shape[1] // 2
    total = 3 * k_steps

    def copies(step):
        phase, k = divmod(step, k_steps)
        slot = step % ahead
        if phase < 2:
            pair, target = ((g0, u0), (g1, u1))[phase], wbuf
            window = lambda w: w.at[0, pl.ds(k * width, width), :]
        else:
            pair, target = (d0, d1), dbuf
            window = lambda w: w.at[0, :, pl.ds(k * width, width)]
        return [
            pltpu.make_async_copy(window(w), target.at[slot, i], wsem.at[slot, i])
            for i, w in enumerate(pair)
        ]

    def piece_copies():
        for i in range(sources):
            s = src_ref[i]
            row = pl.multiple_of((s % 4) * group, group)
            for j in range(4):
                col = pl.multiple_of(((s + (sources - 1 + j)) % sources) * block, block)
                yield pltpu.make_async_copy(
                    parts[2 * i + j // 2].at[:, pl.ds((j % 2) * block, block)],
                    x.at[pl.ds(row, group), pl.ds(col, block)],
                    xsem.at[i, j],
                )

    for c in piece_copies():
        c.start()
    for step in range(ahead):
        for c in copies(step):
            c.start()
    for c in piece_copies():
        c.wait()
    here = src_ref[0]
    own_row = (here % 4) * group + (here // 4) * (group // 4)
    own_ref[...] = x[pl.ds(pl.multiple_of(own_row, group // 4), group // 4), :]

    squares = None
    for k in range(k_steps):
        cols = slice(k * width, (k + 1) * width)
        rows = dot(pick_ref[...], x[:, cols])
        more = jnp.sum(rows * rows, axis=1, keepdims=True)
        squares = more if squares is None else squares + more
        xs[:, cols] = (rows * gain_ref[:, cols]).astype(jnp.bfloat16)
    scale = lax.rsqrt(squares * (1.0 / model) + eps_norm)

    for step in range(total):
        phase, k = divmod(step, k_steps)
        slot = step % ahead
        for c in copies(step):
            c.wait()
        if phase < 2:
            tile = xs[:, k * width : (k + 1) * width]
            g, u = dot(tile, wbuf[slot, 0]), dot(tile, wbuf[slot, 1])
            if k == 0:
                ga[...] = g
                ua[...] = u
            elif k < k_steps - 1:
                ga[...] += g
                ua[...] += u
            else:
                gv, uv = (ga[...] + g) * scale, (ua[...] + u) * scale
                hid[:, phase * ff : (phase + 1) * ff] = (gv / (1.0 + jnp.exp(-gv)) * uv).astype(jnp.bfloat16)
        else:
            rows = dot(hid[:, :ff], dbuf[slot, 0]) + dot(hid[:, ff:], dbuf[slot, 1])
        if step + ahead < total:
            for c in copies(step + ahead):
                c.start()
        if phase == 2:
            out = dot(spread_ref[...], rows.astype(jnp.bfloat16)) * weight_ref[...]
            out_ref[:, k * width : (k + 1) * width] = out.astype(jnp.bfloat16)


def expert_rows(sources, parts, pick, spread, weight, gain, gates0, ups0, gates1, ups1, downs0, downs1):
    rows, tokens = pick.shape
    ff, model = downs0.shape[1:]
    k_steps, ahead = 4, 3
    width = model // k_steps
    count = sources.shape[0]
    return pl.pallas_call(
        functools.partial(expert_kernel, count, k_steps, ahead),
        in_specs=[SMEM] + [ANY] * len(parts) + [VMEM] * 4 + [ANY] * 6,
        out_specs=[VMEM, VMEM],
        out_shape=[
            jax.ShapeDtypeStruct((tokens, model), jnp.bfloat16),
            jax.ShapeDtypeStruct((tokens // count, model), jnp.bfloat16),
        ],
        scratch_shapes=[
            pltpu.VMEM((tokens, model), jnp.bfloat16),
            pltpu.VMEM((ahead, 2, width, ff), jnp.bfloat16),
            pltpu.VMEM((ahead, 2, ff, width), jnp.bfloat16),
            pltpu.SemaphoreType.DMA((ahead, 2)),
            pltpu.SemaphoreType.DMA((count, 4)),
            pltpu.VMEM((rows, model), jnp.bfloat16),
            pltpu.VMEM((rows, ff), jnp.float32),
            pltpu.VMEM((rows, ff), jnp.float32),
            pltpu.VMEM((rows, 2 * ff), jnp.bfloat16),
        ],
        compiler_params=pltpu.CompilerParams(vmem_limit_bytes=56 * 1024 * 1024),
        cost_estimate=pl.CostEstimate(
            flops=12 * rows * model * ff, bytes_accessed=12 * model * ff, transcendentals=2 * rows * ff
        ),
        interpret=INTERPRET,
        name="experts",
    )(sources, *parts, pick, spread, weight, gain, gates0, ups0, gates1, ups1, downs0, downs1)


def rotated(blocks, here):
    return lax.dynamic_slice_in_dim(jnp.concatenate([blocks, blocks], axis=0), here, blocks.shape[0], 0)


def shards(
    hidden,
    queries,
    cache,
    cache_lengths,
    wkv,
    wo,
    attn_gain,
    moe_gain,
    w_gate,
    w_up,
    w_down,
    expert_ids,
    gates,
):
    size = lax.axis_size("tok")
    here = lax.axis_index("tok")
    core = lax.axis_index("mdl")
    cores = lax.axis_size("mdl")
    bf16, f32 = jnp.bfloat16, jnp.float32

    kv_heads, head_dim = wkv.shape[1], wkv.shape[3]
    own_kv = wkv.reshape(wkv.shape[0], -1)
    half = own_kv.shape[0] // 2
    kv_parts, order = [], []
    for i, (source, pair) in enumerate(ring_gather([own_kv[:half], own_kv[half:]])):
        kv_parts += pair
        order.append((-((i + 1) // 2) if i % 2 else i // 2) % size)

    other_hidden = swap(hidden)
    low = jnp.where(core == 0, hidden, other_hidden)
    high = jnp.where(core == 0, other_hidden, hidden)
    full_rows = jnp.concatenate([low, high], axis=1)
    span_len, model = full_rows.shape
    core_rows = span_len // cores
    block = model // size
    normed = rms_scale(full_rows, attn_gain).astype(bf16)
    n_rot = rotated(jnp.moveaxis(normed.reshape(span_len, size, block), 1, 0), here)

    own_rows = lax.dynamic_slice_in_dim(full_rows, core * core_rows, core_rows, 0)
    h_rot = rotated(jnp.moveaxis(own_rows.reshape(core_rows, size, block), 1, 0), here)
    cols = [
        jnp.concatenate([h_rot[size - 1 :], h_rot[:3]], axis=0),
        shift(h_rot[3:7], 4),
        shift(h_rot[size - 5 : size - 1], -4),
        shift(h_rot[7:11], 8),
    ]

    own_wo = wo.reshape(-1, wo.shape[2])
    next_wo = shift(own_wo, -1)
    mine_wo = [shift(own_wo, 1), own_wo, next_wo, shift(next_wo, -1)]
    full_wo = mine_wo + [swap(w) for w in mine_wo]

    other_gate, other_up, other_down = swap(w_gate), swap(w_up), swap(w_down)

    matches = expert_ids[:, :, None] == jnp.arange(EXPERTS)[None, None, :]
    route = jnp.sum(jnp.where(matches, gates[:, :, None], 0.0), axis=1)
    weight = lax.all_to_all(jnp.repeat(route.T, size // EXPERTS, axis=0), "tok", 0, 0, tiled=True)
    weight = jnp.swapaxes(weight.reshape(size // 4, 4, core_rows), 0, 1).reshape(size, core_rows)
    chosen = (weight > 0).astype(jnp.int32)
    rank = jnp.cumsum(chosen, axis=1) - chosen
    capacity = core_rows * TOPK * 9 // (8 * EXPERTS)
    slot = jnp.where(chosen > 0, rank + jnp.arange(size)[:, None] * capacity, -1).reshape(1, -1)
    pick = (jnp.arange(size * capacity)[:, None] == slot).astype(bf16)
    spread = (slot.reshape(-1, 1) == jnp.arange(size * capacity)[None, :]).astype(bf16)

    length = cache_lengths[0]
    head_group = queries.shape[1] // kv_heads
    scale_factor = 1.0 / math.sqrt(head_dim)
    rows = jnp.swapaxes(queries, 0, 1).reshape(kv_heads, head_group * span_len, head_dim)
    keys = jnp.stack([cache[0, :, h, 0] for h in range(kv_heads)])
    values = jnp.stack([cache[0, :, h, 1] for h in range(kv_heads)])
    old = cache_attention(cache_lengths, rows, keys, values, scale_factor)

    positions = (length + jnp.arange(span_len, dtype=jnp.int32)).astype(f32)
    inverse = jnp.exp(
        jnp.arange(head_dim // 2, dtype=f32) * (-2.0 * math.log(rope_base) / head_dim)
    )
    angle = positions[:, None] * inverse[None, :]
    cosine, sine = jnp.cos(angle), jnp.sin(angle)
    heads_out, fresh = fresh_attention(
        kv_parts,
        order,
        n_rot,
        jnp.concatenate([cosine, cosine], axis=1),
        jnp.concatenate([-sine, sine], axis=1),
        rows,
        old,
        scale_factor,
    )
    fresh_key_value = fresh.reshape(span_len, kv_heads, 2, head_dim)

    kept = lax.dynamic_slice_in_dim(heads_out, core * core_rows, core_rows, 0)
    given = lax.dynamic_slice_in_dim(heads_out, (cores - 1 - core) * core_rows, core_rows, 0)
    own_heads = jnp.concatenate([kept, swap(given)], axis=1)
    back, ahead = shift(own_heads, 4), shift(own_heads, -4)
    far = [shift(back[: core_rows // 2], 4), shift(ahead[core_rows // 2 :], -4)]
    places = (here // 4 + jnp.array([0, 3, 1, 2], jnp.int32)) % 4
    left, right = output_rows(places, [own_heads, back, ahead, *far], cols, full_wo)

    parts, sources = [], []
    for source, pair in ring_gather([left, right]):
        parts += pair
        sources.append(source)

    partial, own_resid = expert_rows(
        jnp.stack(sources).astype(jnp.int32),
        parts,
        pick,
        spread,
        weight.reshape(-1, 1),
        moe_gain.astype(f32).reshape(1, -1),
        w_gate,
        w_up,
        other_gate,
        other_up,
        w_down,
        other_down,
    )
    partial = partial.reshape(size, core_rows, model)

    def pieces(device):
        at = (device % 4) * (size // 4) + device // 4
        mine = lax.dynamic_index_in_dim(partial, at, 0, keepdims=False)
        return [mine[:, : model // 2], mine[:, model // 2 :]]

    moe_out = jnp.concatenate(ring_scatter_sum(pieces), axis=1)
    mixed = (own_resid.astype(f32) + moe_out).astype(bf16)
    return (mixed, fresh_key_value)


def solution(mesh):
    in_specs = (
        P(("grp", "tok"), "mdl"),
        P(("grp", "tok"), "mdl", None),
        P(("grp", "tok"), None, "mdl", None, None),
        P(("grp", "tok")),
        P("tok", "mdl", None, None),
        P("mdl", None, "tok"),
        P(),
        P(),
        P(("tok", "mdl"), None, None),
        P(("tok", "mdl"), None, None),
        P(("tok", "mdl"), None, None),
        P(("grp", "tok", "mdl"), None),
        P(("grp", "tok", "mdl"), None),
    )
    out_specs = (P(("grp", "tok", "mdl"), None), P(("grp", "tok"), "mdl", None, None))
    return jax.shard_map(shards, mesh=mesh, in_specs=in_specs, out_specs=out_specs, check_vma=False)
```

```python
import functools
import math

import jax
import jax.numpy as jnp
from jax import lax
from jax.experimental import pallas as pl
from jax.experimental.pallas import tpu as pltpu
from jax.sharding import PartitionSpec as P

EXPERTS = 4
TOPK = 2

eps_norm = 1e-05
rope_base = 1000000.0
mask_fill = -1e30


INTERPRET = False


def shift(x, step):
    size = lax.axis_size("tok")
    return lax.ppermute(x, "tok", [(i, (i + step) % size) for i in range(size)])


def swap(x):
    return lax.ppermute(x, "mdl", [(0, 1), (1, 0)])


def ring_gather(parts, ties=None):
    size = lax.axis_size("tok")
    here = lax.axis_index("tok")
    yield here, parts
    up, down = list(parts), list(parts)
    for step in range(1, size // 2 + 1):
        tie = (ties or {}).get(step)
        if tie:
            up, down, tie[:] = lax.optimization_barrier((up, down, tie))
        up = [shift(p, 1) for p in up]
        last = step == size // 2
        if not last:
            down = [shift(p, -1) for p in down]
        yield (here - step) % size, up
        if not last:
            yield (here + step) % size, down


def ring_scatter_sum(pick):
    size = lax.axis_size("tok")
    here = lax.axis_index("tok")
    half = size // 2

    def joined(arrived, device):
        return [(a.astype(jnp.float32) + b.astype(jnp.float32)) for a, b in zip(arrived, pick(device))]

    up = pick((here + half) % size)
    down = pick((here - half + 1) % size)
    for step in range(1, half + 1):
        up = [shift(p, 1) for p in up]
        if step < half:
            up = [p.astype(jnp.bfloat16) for p in joined(up, (here + half - step) % size)]
            down = [shift(p, -1) for p in down]
            if step < half - 1:
                down = [p.astype(jnp.bfloat16) for p in joined(down, (here - half + 1 + step) % size)]
    own = pick(here)
    return [u.astype(jnp.float32) + d.astype(jnp.float32) + o.astype(jnp.float32) for u, d, o in zip(up, down, own)]


def rms_scale(values_in, gain):
    values = values_in.astype(jnp.float32)
    meansq = jnp.mean(values * values, axis=-1, keepdims=True)
    return values * lax.rsqrt(meansq + eps_norm) * gain.astype(jnp.float32)


def dot(a, b):
    return jnp.dot(a, b, preferred_element_type=jnp.float32)


def score(a, b):
    return lax.dot_general(a, b, (((1,), (1,)), ((), ())), preferred_element_type=jnp.float32)


VMEM = pl.BlockSpec(memory_space=pltpu.VMEM)
SMEM = pl.BlockSpec(memory_space=pltpu.SMEM)
ANY = pl.BlockSpec(memory_space=pl.ANY)


def cache_kernel(scale, length_ref, q_ref, k_ref, v_ref, total_ref, max_ref, sum_ref, s_ref):
    length = length_ref[0]
    block = 512
    steps = k_ref.shape[1] // block
    q = q_ref[0]
    top = None
    for i in range(steps):
        s = score(q, k_ref[0, i * block : (i + 1) * block]) * scale
        column = i * block + lax.broadcasted_iota(jnp.int32, s.shape, 1)
        s = jnp.where(column < length, s, mask_fill)
        s_ref[:, i * block : (i + 1) * block] = s
        high = jnp.max(s, axis=1, keepdims=True)
        top = high if top is None else jnp.maximum(top, high)
    row_sum = jnp.zeros_like(top)
    total = jnp.zeros(total_ref.shape[1:], jnp.float32)
    for i in range(steps):
        s = s_ref[:, i * block : (i + 1) * block]
        column = i * block + lax.broadcasted_iota(jnp.int32, s.shape, 1)
        p = jnp.where(column < length, jnp.exp(s - top), 0.0)
        row_sum += jnp.sum(p, axis=1, keepdims=True)
        total += dot(p.astype(jnp.bfloat16), v_ref[0, i * block : (i + 1) * block])
    total_ref[0] = total
    max_ref[0] = jnp.broadcast_to(top, total.shape)
    sum_ref[0] = jnp.broadcast_to(row_sum, total.shape)


def cache_attention(length, rows, keys, values, scale):
    heads, count, dim = rows.shape
    per_head = lambda n: pl.BlockSpec((1, n, dim), lambda i: (i, 0, 0))
    out = jax.ShapeDtypeStruct((heads, count, dim), jnp.float32)
    return pl.pallas_call(
        functools.partial(cache_kernel, scale),
        grid=(heads,),
        in_specs=[SMEM, per_head(count), per_head(keys.shape[1]), per_head(keys.shape[1])],
        out_specs=[per_head(count)] * 3,
        out_shape=[out] * 3,
        scratch_shapes=[pltpu.VMEM((count, keys.shape[1]), jnp.float32)],
        compiler_params=pltpu.CompilerParams(
            dimension_semantics=("arbitrary",), vmem_limit_bytes=16 * 1024 * 1024
        ),
        cost_estimate=pl.CostEstimate(
            flops=4 * heads * count * dim * keys.shape[1],
            bytes_accessed=4 * keys.size,
            transcendentals=heads * count * keys.shape[1],
        ),
        interpret=INTERPRET,
        name="cache_attention",
    )(length, rows, keys, values)


def fresh_kernel(scale, order, *refs):
    parts = refs[: 2 * len(order)]
    n_ref, cos_ref, sin_ref, q_ref, total_ref, max_ref, sum_ref, heads_ref, fresh_ref = refs[2 * len(order) :]
    half = n_ref.shape[2] // 2
    span = n_ref.shape[1]
    kv = None
    for i, at in enumerate(order):
        more = dot(n_ref[at, :, :half], parts[2 * i][:half]) + dot(n_ref[at, :, half:], parts[2 * i + 1][...])
        kv = more if kv is None else kv + more
    heads, count, dim = q_ref.shape
    group = count // span
    for h in range(heads):
        k = kv[:, 2 * h * dim : (2 * h + 1) * dim]
        v = kv[:, (2 * h + 1) * dim : (2 * h + 2) * dim].astype(jnp.bfloat16)
        k = (k * cos_ref[...] + pltpu.roll(k, dim // 2, 1) * sin_ref[...]).astype(jnp.bfloat16)
        fresh_ref[:, 2 * h * dim : (2 * h + 1) * dim] = k
        fresh_ref[:, (2 * h + 1) * dim : (2 * h + 2) * dim] = v
        s = score(q_ref[h], k) * scale
        token = lax.broadcasted_iota(jnp.int32, s.shape, 0) % span
        allowed = lax.broadcasted_iota(jnp.int32, s.shape, 1) <= token
        s = jnp.where(allowed, s, mask_fill)
        old_max = max_ref[h][:, :1]
        top = jnp.maximum(old_max, jnp.max(s, axis=1, keepdims=True))
        p = jnp.where(allowed, jnp.exp(s - top), 0.0)
        decay = jnp.exp(old_max - top)
        row_sum = sum_ref[h][:, :1] * decay + jnp.sum(p, axis=1, keepdims=True)
        out = (total_ref[h] * decay + dot(p.astype(jnp.bfloat16), v)) / row_sum
        for g in range(group):
            col = (h * group + g) * dim
            heads_ref[:, col : col + dim] = out[g * span : (g + 1) * span].astype(jnp.bfloat16)


def fresh_attention(parts, order, n_rot, cosine, sine, rows, old, scale):
    span = n_rot.shape[1]
    heads, count, dim = rows.shape
    return pl.pallas_call(
        functools.partial(fresh_kernel, scale, order),
        in_specs=[VMEM] * (len(parts) + 7),
        out_specs=[VMEM, VMEM],
        out_shape=[
            jax.ShapeDtypeStruct((span, heads * (count // span) * dim), jnp.bfloat16),
            jax.ShapeDtypeStruct((span, heads * 2 * dim), jnp.bfloat16),
        ],
        compiler_params=pltpu.CompilerParams(vmem_limit_bytes=24 * 1024 * 1024),
        interpret=INTERPRET,
        name="fresh_attention",
    )(*parts, n_rot, cosine, sine, rows, *old)


def output_kernel(places_ref, h0, h1, h2, h3a, h3b, c0, c1, c2, c3, *refs):
    weights = refs[:8]
    left_ref, right_ref, all_ref = refs[8:]
    n = h0.shape[0]
    all_ref[0:n] = h0[...]
    all_ref[n : 2 * n] = h1[...]
    all_ref[2 * n : 3 * n] = h2[...]
    all_ref[3 * n : 3 * n + n // 2] = h3a[...]
    all_ref[3 * n + n // 2 :] = h3b[...]
    half = all_ref.shape[1] // 2
    mine, other = all_ref[:, :half], all_ref[:, half:]
    block = c0.shape[2]
    for j in range(4):
        out = dot(mine, weights[j][...]) + dot(other, weights[4 + j][...])
        target = left_ref if j < 2 else right_ref
        for g, c in enumerate((c0, c1, c2, c3)):
            row = pl.multiple_of(places_ref[g] * n, n)
            value = out[g * n : (g + 1) * n] + c[j].astype(jnp.float32)
            target[pl.ds(row, n), (j % 2) * block : (j % 2 + 1) * block] = value.astype(jnp.bfloat16)


def output_rows(places, heads, cols, weights):
    n, width = heads[0].shape
    block = cols[0].shape[2]
    out = jax.ShapeDtypeStruct((4 * n, 2 * block), jnp.bfloat16)
    return pl.pallas_call(
        output_kernel,
        in_specs=[SMEM] + [VMEM] * 17,
        out_specs=[VMEM, VMEM],
        out_shape=[out, out],
        scratch_shapes=[pltpu.VMEM((4 * n, width), jnp.bfloat16)],
        compiler_params=pltpu.CompilerParams(vmem_limit_bytes=24 * 1024 * 1024),
        interpret=INTERPRET,
        name="output_rows",
    )(places, *heads, *cols, *weights)


def expert_kernel(sources, k_steps, ahead, src_ref, *refs):
    parts = refs[: 2 * sources]
    (pick_ref, spread_ref, weight_ref, gain_ref, g0, u0, g1, u1, d0, d1, out_ref, own_ref,
     x, wbuf, dbuf, wsem, xsem, xs, ga, ua, hid) = refs[2 * sources :]
    model = x.shape[1]
    ff = ga.shape[1]
    width = model // k_steps
    group = parts[0].shape[0]
    block = parts[0].shape[1] // 2
    total = 3 * k_steps

    def copies(step):
        phase, k = divmod(step, k_steps)
        slot = step % ahead if phase < 2 else k
        if phase < 2:
            pair, target = ((g0, u0), (g1, u1))[phase], wbuf
            window = lambda w: w.at[0, pl.ds(k * width, width), :]
        else:
            pair, target = (d0, d1), dbuf
            window = lambda w: w.at[0, :, pl.ds(k * width, width)]
        return [
            pltpu.make_async_copy(window(w), target.at[slot, i], wsem.at[step, i])
            for i, w in enumerate(pair)
        ]

    def piece_copies():
        for i in range(sources):
            s = src_ref[i]
            row = pl.multiple_of((s % 4) * group, group)
            for j in range(4):
                col = pl.multiple_of(((s + (sources - 1 + j)) % sources) * block, block)
                yield pltpu.make_async_copy(
                    parts[2 * i + j // 2].at[:, pl.ds((j % 2) * block, block)],
                    x.at[pl.ds(row, group), pl.ds(col, block)],
                    xsem.at[i, j],
                )

    for c in piece_copies():
        c.start()
    for step in range(ahead):
        for c in copies(step):
            c.start()
    for c in piece_copies():
        c.wait()
    here = src_ref[0]
    own_row = (here % 4) * group + (here // 4) * (group // 4)
    own_ref[...] = x[pl.ds(pl.multiple_of(own_row, group // 4), group // 4), :]

    squares = None
    for k in range(k_steps):
        cols = slice(k * width, (k + 1) * width)
        rows = dot(pick_ref[...], x[:, cols])
        more = jnp.sum(rows * rows, axis=1, keepdims=True)
        squares = more if squares is None else squares + more
        xs[:, cols] = (rows * gain_ref[:, cols]).astype(jnp.bfloat16)
    scale = lax.rsqrt(squares * (1.0 / model) + eps_norm)

    for step in range(total):
        phase, k = divmod(step, k_steps)
        slot = step % ahead if phase < 2 else k
        for c in copies(step):
            c.wait()
        if phase < 2:
            tile = xs[:, k * width : (k + 1) * width]
            g, u = dot(tile, wbuf[slot, 0]), dot(tile, wbuf[slot, 1])
            if k == 0:
                ga[...] = g
                ua[...] = u
            elif k < k_steps - 1:
                ga[...] += g
                ua[...] += u
            else:
                gv, uv = (ga[...] + g) * scale, (ua[...] + u) * scale
                hid[:, phase * ff : (phase + 1) * ff] = (gv / (1.0 + jnp.exp(-gv)) * uv).astype(jnp.bfloat16)
        else:
            rows = dot(hid[:, :ff], dbuf[slot, 0]) + dot(hid[:, ff:], dbuf[slot, 1])
        if step + ahead < total:
            for c in copies(step + ahead):
                c.start()
        if phase == 2:
            out = dot(spread_ref[...], rows.astype(jnp.bfloat16)) * weight_ref[...]
            out_ref[:, k * width : (k + 1) * width] = out.astype(jnp.bfloat16)


def expert_rows(sources, parts, pick, spread, weight, gain, gates0, ups0, gates1, ups1, downs0, downs1):
    rows, tokens = pick.shape
    ff, model = downs0.shape[1:]
    k_steps, ahead = 4, 3
    width = model // k_steps
    count = sources.shape[0]
    return pl.pallas_call(
        functools.partial(expert_kernel, count, k_steps, ahead),
        in_specs=[SMEM] + [ANY] * len(parts) + [VMEM] * 4 + [ANY] * 6,
        out_specs=[VMEM, VMEM],
        out_shape=[
            jax.ShapeDtypeStruct((tokens, model), jnp.bfloat16),
            jax.ShapeDtypeStruct((tokens // count, model), jnp.bfloat16),
        ],
        scratch_shapes=[
            pltpu.VMEM((tokens, model), jnp.bfloat16),
            pltpu.VMEM((ahead, 2, width, ff), jnp.bfloat16),
            pltpu.VMEM((k_steps, 2, ff, width), jnp.bfloat16),
            pltpu.SemaphoreType.DMA((3 * k_steps, 2)),
            pltpu.SemaphoreType.DMA((count, 4)),
            pltpu.VMEM((rows, model), jnp.bfloat16),
            pltpu.VMEM((rows, ff), jnp.float32),
            pltpu.VMEM((rows, ff), jnp.float32),
            pltpu.VMEM((rows, 2 * ff), jnp.bfloat16),
        ],
        compiler_params=pltpu.CompilerParams(vmem_limit_bytes=46 * 1024 * 1024),
        cost_estimate=pl.CostEstimate(
            flops=12 * rows * model * ff, bytes_accessed=12 * model * ff, transcendentals=2 * rows * ff
        ),
        interpret=INTERPRET,
        name="experts",
    )(sources, *parts, pick, spread, weight, gain, gates0, ups0, gates1, ups1, downs0, downs1)


def rotated(blocks, here):
    return lax.dynamic_slice_in_dim(jnp.concatenate([blocks, blocks], axis=0), here, blocks.shape[0], 0)


def shards(
    hidden,
    queries,
    cache,
    cache_lengths,
    wkv,
    wo,
    attn_gain,
    moe_gain,
    w_gate,
    w_up,
    w_down,
    expert_ids,
    gates,
):
    size = lax.axis_size("tok")
    here = lax.axis_index("tok")
    core = lax.axis_index("mdl")
    cores = lax.axis_size("mdl")
    bf16, f32 = jnp.bfloat16, jnp.float32

    other_hidden = swap(hidden)
    low = jnp.where(core == 0, hidden, other_hidden)
    high = jnp.where(core == 0, other_hidden, hidden)
    full_rows = jnp.concatenate([low, high], axis=1)
    span_len, model = full_rows.shape
    core_rows = span_len // cores
    block = model // size
    normed = rms_scale(full_rows, attn_gain).astype(bf16)
    n_rot = rotated(jnp.moveaxis(normed.reshape(span_len, size, block), 1, 0), here)

    own_rows = lax.dynamic_slice_in_dim(full_rows, core * core_rows, core_rows, 0)
    h_rot = rotated(jnp.moveaxis(own_rows.reshape(core_rows, size, block), 1, 0), here)
    cols = [
        jnp.concatenate([h_rot[size - 1 :], h_rot[:3]], axis=0),
        shift(h_rot[3:7], 4),
        shift(h_rot[size - 5 : size - 1], -4),
        shift(h_rot[7:11], 8),
    ]

    own_wo = wo.reshape(-1, wo.shape[2])
    next_wo = shift(own_wo, -1)
    mine_wo = [shift(own_wo, 1), own_wo, next_wo, shift(next_wo, -1)]
    full_wo = mine_wo + [swap(w) for w in mine_wo]

    matches = expert_ids[:, :, None] == jnp.arange(EXPERTS)[None, None, :]
    route = jnp.sum(jnp.where(matches, gates[:, :, None], 0.0), axis=1).T
    coarse = lax.reduce_precision(route, 8, 7)
    note = jnp.concatenate([coarse, route - coarse], axis=0).astype(bf16).reshape(1, -1)
    kv_heads, head_dim = wkv.shape[1], wkv.shape[3]
    own_kv = wkv.reshape(wkv.shape[0], -1)
    half = own_kv.shape[0] // 2
    note = jnp.pad(note, ((0, 7), (0, own_kv.shape[1] - note.shape[1])))
    kv_parts, order = [], []
    ties = {3: cols[1:], size // 2: full_wo[4:]}
    ring = ring_gather([jnp.concatenate([own_kv[:half], note], axis=0), own_kv[half:]], ties)
    for i, (source, pair) in enumerate(ring):
        kv_parts += pair
        order.append((-((i + 1) // 2) if i % 2 else i // 2) % size)
    cols = cols[:1] + ties[3]
    full_wo = full_wo[:4] + ties[size // 2]

    count = EXPERTS * core_rows
    notes = [None] * size
    for i, at in enumerate(order):
        notes[at] = kv_parts[2 * i][half : half + 1, : 2 * count]
    notes = rotated(jnp.concatenate(notes, axis=0), (size - here) % size)
    notes = notes.reshape(size, 2, EXPERTS, core_rows).astype(f32)
    weight = lax.dynamic_index_in_dim(notes[:, 0] + notes[:, 1], here * EXPERTS // size, 1, keepdims=False)
    weight = jnp.swapaxes(weight.reshape(size // 4, 4, core_rows), 0, 1).reshape(size, core_rows)
    chosen = (weight > 0).astype(jnp.int32)
    rank = jnp.cumsum(chosen, axis=1) - chosen
    capacity = core_rows * TOPK * 9 // (8 * EXPERTS)
    slot = jnp.where(chosen > 0, rank + jnp.arange(size)[:, None] * capacity, -1).reshape(1, -1)
    pick = (jnp.arange(size * capacity)[:, None] == slot).astype(bf16)
    spread = (slot.reshape(-1, 1) == jnp.arange(size * capacity)[None, :]).astype(bf16)

    other_gate, other_up, other_down = swap(w_gate), swap(w_up), swap(w_down)

    length = cache_lengths[0]
    head_group = queries.shape[1] // kv_heads
    scale_factor = 1.0 / math.sqrt(head_dim)
    rows = jnp.swapaxes(queries, 0, 1).reshape(kv_heads, head_group * span_len, head_dim)
    keys = jnp.stack([cache[0, :, h, 0] for h in range(kv_heads)])
    values = jnp.stack([cache[0, :, h, 1] for h in range(kv_heads)])
    old = cache_attention(cache_lengths, rows, keys, values, scale_factor)

    positions = (length + jnp.arange(span_len, dtype=jnp.int32)).astype(f32)
    inverse = jnp.exp(
        jnp.arange(head_dim // 2, dtype=f32) * (-2.0 * math.log(rope_base) / head_dim)
    )
    angle = positions[:, None] * inverse[None, :]
    cosine, sine = jnp.cos(angle), jnp.sin(angle)
    heads_out, fresh = fresh_attention(
        kv_parts,
        order,
        n_rot,
        jnp.concatenate([cosine, cosine], axis=1),
        jnp.concatenate([-sine, sine], axis=1),
        rows,
        old,
        scale_factor,
    )
    fresh_key_value = fresh.reshape(span_len, kv_heads, 2, head_dim)

    kept = lax.dynamic_slice_in_dim(heads_out, core * core_rows, core_rows, 0)
    given = lax.dynamic_slice_in_dim(heads_out, (cores - 1 - core) * core_rows, core_rows, 0)
    own_heads = jnp.concatenate([kept, swap(given)], axis=1)
    back, ahead = shift(own_heads, 4), shift(own_heads, -4)
    far = [shift(back[: core_rows // 2], 4), shift(ahead[core_rows // 2 :], -4)]
    places = (here // 4 + jnp.array([0, 3, 1, 2], jnp.int32)) % 4
    left, right = output_rows(places, [own_heads, back, ahead, *far], cols, full_wo)

    parts, sources = [], []
    for source, pair in ring_gather([left, right]):
        parts += pair
        sources.append(source)

    partial, own_resid = expert_rows(
        jnp.stack(sources).astype(jnp.int32),
        parts,
        pick,
        spread,
        weight.reshape(-1, 1),
        moe_gain.astype(f32).reshape(1, -1),
        w_gate,
        w_up,
        other_gate,
        other_up,
        w_down,
        other_down,
    )
    partial = partial.reshape(size, core_rows, model)

    def pieces(device):
        at = (device % 4) * (size // 4) + device // 4
        mine = lax.dynamic_index_in_dim(partial, at, 0, keepdims=False)
        return [mine[:, : model // 2], mine[:, model // 2 :]]

    moe_out = jnp.concatenate(ring_scatter_sum(pieces), axis=1)
    mixed = (own_resid.astype(f32) + moe_out).astype(bf16)
    return (mixed, fresh_key_value)


def solution(mesh):
    in_specs = (
        P(("grp", "tok"), "mdl"),
        P(("grp", "tok"), "mdl", None),
        P(("grp", "tok"), None, "mdl", None, None),
        P(("grp", "tok")),
        P("tok", "mdl", None, None),
        P("mdl", None, "tok"),
        P(),
        P(),
        P(("tok", "mdl"), None, None),
        P(("tok", "mdl"), None, None),
        P(("tok", "mdl"), None, None),
        P(("grp", "tok", "mdl"), None),
        P(("grp", "tok", "mdl"), None),
    )
    out_specs = (P(("grp", "tok", "mdl"), None), P(("grp", "tok"), "mdl", None, None))
    return jax.shard_map(shards, mesh=mesh, in_specs=in_specs, out_specs=out_specs, check_vma=False)
```

```python
import functools
import math

import jax
import jax.numpy as jnp
from jax import lax
from jax.experimental import pallas as pl
from jax.experimental.pallas import tpu as pltpu
from jax.sharding import PartitionSpec as P

EXPERTS = 4
TOPK = 2

eps_norm = 1e-05
rope_base = 1000000.0
mask_fill = -1e30


INTERPRET = False


def shift(x, step):
    size = lax.axis_size("tok")
    return lax.ppermute(x, "tok", [(i, (i + step) % size) for i in range(size)])


def swap(x):
    return lax.ppermute(x, "mdl", [(0, 1), (1, 0)])


def rms_scale(values_in, gain):
    values = values_in.astype(jnp.float32)
    meansq = jnp.mean(values * values, axis=-1, keepdims=True)
    return values * lax.rsqrt(meansq + eps_norm) * gain.astype(jnp.float32)


def dot(a, b):
    return jnp.dot(a, b, preferred_element_type=jnp.float32)


def score(a, b):
    return lax.dot_general(a, b, (((1,), (1,)), ((), ())), preferred_element_type=jnp.float32)


VMEM = pl.BlockSpec(memory_space=pltpu.VMEM)
SMEM = pl.BlockSpec(memory_space=pltpu.SMEM)
ANY = pl.BlockSpec(memory_space=pl.ANY)


def cache_kernel(scale, length_ref, q_ref, k_ref, v_ref, total_ref, max_ref, sum_ref, s_ref):
    length = length_ref[0]
    block = 512
    steps = k_ref.shape[1] // block
    q = q_ref[0]
    top = None
    for i in range(steps):
        s = score(q, k_ref[0, i * block : (i + 1) * block]) * scale
        column = i * block + lax.broadcasted_iota(jnp.int32, s.shape, 1)
        s = jnp.where(column < length, s, mask_fill)
        s_ref[:, i * block : (i + 1) * block] = s
        high = jnp.max(s, axis=1, keepdims=True)
        top = high if top is None else jnp.maximum(top, high)
    row_sum = jnp.zeros_like(top)
    total = jnp.zeros(total_ref.shape[1:], jnp.float32)
    for i in range(steps):
        s = s_ref[:, i * block : (i + 1) * block]
        column = i * block + lax.broadcasted_iota(jnp.int32, s.shape, 1)
        p = jnp.where(column < length, jnp.exp(s - top), 0.0)
        row_sum += jnp.sum(p, axis=1, keepdims=True)
        total += dot(p.astype(jnp.bfloat16), v_ref[0, i * block : (i + 1) * block])
    total_ref[0] = total
    max_ref[0] = jnp.broadcast_to(top, total.shape)
    sum_ref[0] = jnp.broadcast_to(row_sum, total.shape)


def cache_attention(length, rows, keys, values, scale):
    heads, count, dim = rows.shape
    per_head = lambda n: pl.BlockSpec((1, n, dim), lambda i: (i, 0, 0))
    out = jax.ShapeDtypeStruct((heads, count, dim), jnp.float32)
    return pl.pallas_call(
        functools.partial(cache_kernel, scale),
        grid=(heads,),
        in_specs=[SMEM, per_head(count), per_head(keys.shape[1]), per_head(keys.shape[1])],
        out_specs=[per_head(count)] * 3,
        out_shape=[out] * 3,
        scratch_shapes=[pltpu.VMEM((count, keys.shape[1]), jnp.float32)],
        compiler_params=pltpu.CompilerParams(
            dimension_semantics=("arbitrary",), vmem_limit_bytes=16 * 1024 * 1024
        ),
        cost_estimate=pl.CostEstimate(
            flops=4 * heads * count * dim * keys.shape[1],
            bytes_accessed=4 * keys.size,
            transcendentals=heads * count * keys.shape[1],
        ),
        interpret=INTERPRET,
        name="cache_attention",
    )(length, rows, keys, values)


def fresh_kernel(scale, n_ref, w_ref, cos_ref, sin_ref, q_ref, total_ref, max_ref, sum_ref, heads_ref, fresh_ref):
    span = n_ref.shape[0]
    kv = dot(n_ref[...], w_ref[...])
    heads, count, dim = q_ref.shape
    group = count // span
    for h in range(heads):
        k = kv[:, 2 * h * dim : (2 * h + 1) * dim]
        v = kv[:, (2 * h + 1) * dim : (2 * h + 2) * dim].astype(jnp.bfloat16)
        k = (k * cos_ref[...] + pltpu.roll(k, dim // 2, 1) * sin_ref[...]).astype(jnp.bfloat16)
        fresh_ref[:, 2 * h * dim : (2 * h + 1) * dim] = k
        fresh_ref[:, (2 * h + 1) * dim : (2 * h + 2) * dim] = v
        s = score(q_ref[h], k) * scale
        token = lax.broadcasted_iota(jnp.int32, s.shape, 0) % span
        allowed = lax.broadcasted_iota(jnp.int32, s.shape, 1) <= token
        s = jnp.where(allowed, s, mask_fill)
        old_max = max_ref[h][:, :1]
        top = jnp.maximum(old_max, jnp.max(s, axis=1, keepdims=True))
        p = jnp.where(allowed, jnp.exp(s - top), 0.0)
        decay = jnp.exp(old_max - top)
        row_sum = sum_ref[h][:, :1] * decay + jnp.sum(p, axis=1, keepdims=True)
        out = (total_ref[h] * decay + dot(p.astype(jnp.bfloat16), v)) / row_sum
        for g in range(group):
            col = (h * group + g) * dim
            heads_ref[:, col : col + dim] = out[g * span : (g + 1) * span].astype(jnp.bfloat16)


def fresh_attention(normed, weights, cosine, sine, rows, old, scale):
    span = normed.shape[0]
    heads, count, dim = rows.shape
    return pl.pallas_call(
        functools.partial(fresh_kernel, scale),
        in_specs=[VMEM] * 8,
        out_specs=[VMEM, VMEM],
        out_shape=[
            jax.ShapeDtypeStruct((span, heads * (count // span) * dim), jnp.bfloat16),
            jax.ShapeDtypeStruct((span, heads * 2 * dim), jnp.bfloat16),
        ],
        compiler_params=pltpu.CompilerParams(vmem_limit_bytes=24 * 1024 * 1024),
        interpret=INTERPRET,
        name="fresh_attention",
    )(normed, weights, cosine, sine, rows, *old)


def output_kernel(places_ref, h0, h1, h2, h3a, h3b, c0, c1, c2, c3, *refs):
    weights = refs[:8]
    out_ref, all_ref = refs[8:]
    n = h0.shape[0]
    all_ref[0:n] = h0[...]
    all_ref[n : 2 * n] = h1[...]
    all_ref[2 * n : 3 * n] = h2[...]
    all_ref[3 * n : 3 * n + n // 2] = h3a[...]
    all_ref[3 * n + n // 2 :] = h3b[...]
    half = all_ref.shape[1] // 2
    mine, other = all_ref[:, :half], all_ref[:, half:]
    block = c0.shape[2]
    for j in range(4):
        out = dot(mine, weights[j][...]) + dot(other, weights[4 + j][...])
        for g, c in enumerate((c0, c1, c2, c3)):
            row = pl.multiple_of(places_ref[g] * n, n)
            value = out[g * n : (g + 1) * n] + c[j].astype(jnp.float32)
            out_ref[pl.ds(row, n), j * block : (j + 1) * block] = value.astype(jnp.bfloat16)


def output_rows(places, heads, cols, weights):
    n, width = heads[0].shape
    block = cols[0].shape[2]
    return pl.pallas_call(
        output_kernel,
        in_specs=[SMEM] + [VMEM] * 17,
        out_specs=VMEM,
        out_shape=jax.ShapeDtypeStruct((4 * n, 4 * block), jnp.bfloat16),
        scratch_shapes=[pltpu.VMEM((4 * n, width), jnp.bfloat16)],
        compiler_params=pltpu.CompilerParams(vmem_limit_bytes=24 * 1024 * 1024),
        interpret=INTERPRET,
        name="output_rows",
    )(places, *heads, *cols, *weights)


def expert_kernel(sources, k_steps, ahead, here_ref, parts, *refs):
    (pick_ref, spread_ref, weight_ref, gain_ref, g0, u0, g1, u1, d0, d1, out_ref, own_ref,
     x, wbuf, dbuf, wsem, xsem, xs, ga, ua, hid) = refs
    model = x.shape[1]
    ff = ga.shape[1]
    width = model // k_steps
    group = parts.shape[0] // sources
    block = parts.shape[1] // 4
    total = 3 * k_steps

    def copies(step):
        phase, k = divmod(step, k_steps)
        slot = step % ahead if phase < 2 else k
        if phase < 2:
            pair, target = ((g0, u0), (g1, u1))[phase], wbuf
            window = lambda w: w.at[0, pl.ds(k * width, width), :]
        else:
            pair, target = (d0, d1), dbuf
            window = lambda w: w.at[0, :, pl.ds(k * width, width)]
        return [
            pltpu.make_async_copy(window(w), target.at[slot, i], wsem.at[step, i])
            for i, w in enumerate(pair)
        ]

    def piece_copies():
        for i in range(sources):
            for j in range(4):
                yield pltpu.make_async_copy(
                    parts.at[pl.ds(i * group, group), pl.ds(j * block, block)],
                    x.at[pl.ds((i % 4) * group, group), pl.ds((i + sources - 1 + j) % sources * block, block)],
                    xsem.at[i, j],
                )

    for c in piece_copies():
        c.start()
    for step in range(ahead):
        for c in copies(step):
            c.start()
    for c in piece_copies():
        c.wait()
    here = here_ref[0]
    own_row = (here % 4) * group + (here // 4) * (group // 4)
    own_ref[...] = x[pl.ds(pl.multiple_of(own_row, group // 4), group // 4), :]

    squares = None
    for k in range(k_steps):
        cols = slice(k * width, (k + 1) * width)
        rows = dot(pick_ref[...], x[:, cols])
        more = jnp.sum(rows * rows, axis=1, keepdims=True)
        squares = more if squares is None else squares + more
        xs[:, cols] = (rows * gain_ref[:, cols]).astype(jnp.bfloat16)
    scale = lax.rsqrt(squares * (1.0 / model) + eps_norm)

    for step in range(total):
        phase, k = divmod(step, k_steps)
        slot = step % ahead if phase < 2 else k
        for c in copies(step):
            c.wait()
        if phase < 2:
            tile = xs[:, k * width : (k + 1) * width]
            g, u = dot(tile, wbuf[slot, 0]), dot(tile, wbuf[slot, 1])
            if k == 0:
                ga[...] = g
                ua[...] = u
            elif k < k_steps - 1:
                ga[...] += g
                ua[...] += u
            else:
                gv, uv = (ga[...] + g) * scale, (ua[...] + u) * scale
                hid[:, phase * ff : (phase + 1) * ff] = (gv / (1.0 + jnp.exp(-gv)) * uv).astype(jnp.bfloat16)
        else:
            rows = dot(hid[:, :ff], dbuf[slot, 0]) + dot(hid[:, ff:], dbuf[slot, 1])
        if step + ahead < total:
            for c in copies(step + ahead):
                c.start()
        if phase == 2:
            out = dot(spread_ref[...], rows.astype(jnp.bfloat16)) * weight_ref[...]
            out_ref[:, k * width : (k + 1) * width] = out.astype(jnp.bfloat16)


def expert_rows(size, here, parts, pick, spread, weight, gain, gates0, ups0, gates1, ups1, downs0, downs1):
    rows, tokens = pick.shape
    ff, model = downs0.shape[1:]
    k_steps, ahead = 4, 3
    width = model // k_steps
    count = size
    return pl.pallas_call(
        functools.partial(expert_kernel, count, k_steps, ahead),
        in_specs=[SMEM] + [ANY] + [VMEM] * 4 + [ANY] * 6,
        out_specs=[VMEM, VMEM],
        out_shape=[
            jax.ShapeDtypeStruct((tokens, model), jnp.bfloat16),
            jax.ShapeDtypeStruct((tokens // count, model), jnp.bfloat16),
        ],
        scratch_shapes=[
            pltpu.VMEM((tokens, model), jnp.bfloat16),
            pltpu.VMEM((ahead, 2, width, ff), jnp.bfloat16),
            pltpu.VMEM((k_steps, 2, ff, width), jnp.bfloat16),
            pltpu.SemaphoreType.DMA((3 * k_steps, 2)),
            pltpu.SemaphoreType.DMA((count, 4)),
            pltpu.VMEM((rows, model), jnp.bfloat16),
            pltpu.VMEM((rows, ff), jnp.float32),
            pltpu.VMEM((rows, ff), jnp.float32),
            pltpu.VMEM((rows, 2 * ff), jnp.bfloat16),
        ],
        compiler_params=pltpu.CompilerParams(vmem_limit_bytes=46 * 1024 * 1024),
        cost_estimate=pl.CostEstimate(
            flops=12 * rows * model * ff, bytes_accessed=12 * model * ff, transcendentals=2 * rows * ff
        ),
        interpret=INTERPRET,
        name="experts",
    )(here, parts, pick, spread, weight, gain, gates0, ups0, gates1, ups1, downs0, downs1)


def rotated(blocks, here):
    return lax.dynamic_slice_in_dim(jnp.concatenate([blocks, blocks], axis=0), here, blocks.shape[0], 0)


def shards(
    hidden,
    queries,
    cache,
    cache_lengths,
    wkv,
    wo,
    attn_gain,
    moe_gain,
    w_gate,
    w_up,
    w_down,
    expert_ids,
    gates,
):
    size = lax.axis_size("tok")
    here = lax.axis_index("tok")
    core = lax.axis_index("mdl")
    cores = lax.axis_size("mdl")
    bf16, f32 = jnp.bfloat16, jnp.float32

    kv_heads, head_dim = wkv.shape[1], wkv.shape[3]
    kv_weights = lax.all_gather(wkv.reshape(wkv.shape[0], -1), "tok", axis=0, tiled=True)

    other_hidden = swap(hidden)
    low = jnp.where(core == 0, hidden, other_hidden)
    high = jnp.where(core == 0, other_hidden, hidden)
    full_rows = jnp.concatenate([low, high], axis=1)
    span_len, model = full_rows.shape
    core_rows = span_len // cores
    block = model // size
    normed = rms_scale(full_rows, attn_gain).astype(bf16)

    own_rows = lax.dynamic_slice_in_dim(full_rows, core * core_rows, core_rows, 0)
    h_rot = rotated(jnp.moveaxis(own_rows.reshape(core_rows, size, block), 1, 0), here)
    cols = [
        jnp.concatenate([h_rot[size - 1 :], h_rot[:3]], axis=0),
        shift(h_rot[3:7], 4),
        shift(h_rot[size - 5 : size - 1], -4),
        shift(h_rot[7:11], 8),
    ]

    own_wo = wo.reshape(-1, wo.shape[2])
    next_wo = shift(own_wo, -1)
    mine_wo = [shift(own_wo, 1), own_wo, next_wo, shift(next_wo, -1)]
    full_wo = mine_wo + [swap(w) for w in mine_wo]

    other_gate, other_up, other_down = swap(w_gate), swap(w_up), swap(w_down)

    matches = expert_ids[:, :, None] == jnp.arange(EXPERTS)[None, None, :]
    route = jnp.sum(jnp.where(matches, gates[:, :, None], 0.0), axis=1)
    weight = lax.all_to_all(jnp.repeat(route.T, size // EXPERTS, axis=0), "tok", 0, 0, tiled=True)
    weight = weight.reshape(size, core_rows)
    chosen = (weight > 0).astype(jnp.int32)
    rank = jnp.cumsum(chosen, axis=1) - chosen
    capacity = core_rows * TOPK * 9 // (8 * EXPERTS)
    slot = jnp.where(chosen > 0, rank + jnp.arange(size)[:, None] * capacity, -1)
    slots = jnp.arange(size * capacity)
    by_class = jnp.swapaxes(slot.reshape(size // 4, 4, core_rows), 0, 1)
    pick = (slots[:, None] == by_class.reshape(1, -1)).astype(bf16)
    spread = (slot.reshape(-1, 1) == slots[None, :]).astype(bf16)
    weight = weight.reshape(-1, 1)

    length = cache_lengths[0]
    head_group = queries.shape[1] // kv_heads
    scale_factor = 1.0 / math.sqrt(head_dim)
    rows = jnp.swapaxes(queries, 0, 1).reshape(kv_heads, head_group * span_len, head_dim)
    keys = jnp.stack([cache[0, :, h, 0] for h in range(kv_heads)])
    values = jnp.stack([cache[0, :, h, 1] for h in range(kv_heads)])
    old = cache_attention(cache_lengths, rows, keys, values, scale_factor)

    kv_weights, cols[1:], pick, spread, weight = lax.optimization_barrier(
        (kv_weights, cols[1:], pick, spread, weight)
    )
    positions = (length + jnp.arange(span_len, dtype=jnp.int32)).astype(f32)
    inverse = jnp.exp(
        jnp.arange(head_dim // 2, dtype=f32) * (-2.0 * math.log(rope_base) / head_dim)
    )
    angle = positions[:, None] * inverse[None, :]
    cosine, sine = jnp.cos(angle), jnp.sin(angle)
    heads_out, fresh = fresh_attention(
        normed,
        kv_weights,
        jnp.concatenate([cosine, cosine], axis=1),
        jnp.concatenate([-sine, sine], axis=1),
        rows,
        old,
        scale_factor,
    )
    fresh_key_value = fresh.reshape(span_len, kv_heads, 2, head_dim)

    kept = lax.dynamic_slice_in_dim(heads_out, core * core_rows, core_rows, 0)
    given = lax.dynamic_slice_in_dim(heads_out, (cores - 1 - core) * core_rows, core_rows, 0)
    own_heads = jnp.concatenate([kept, swap(given)], axis=1)
    back, ahead = shift(own_heads, 4), shift(own_heads, -4)
    far = [shift(back[: core_rows // 2], 4), shift(ahead[core_rows // 2 :], -4)]
    places = (here // 4 + jnp.array([0, 3, 1, 2], jnp.int32)) % 4
    resid_cols = output_rows(places, [own_heads, back, ahead, *far], cols, full_wo)

    resid_all = lax.all_gather(resid_cols, "tok", axis=0, tiled=True)

    partial, own_resid = expert_rows(
        size,
        here.reshape(1).astype(jnp.int32),
        resid_all,
        pick,
        spread,
        weight,
        moe_gain.astype(f32).reshape(1, -1),
        w_gate,
        w_up,
        other_gate,
        other_up,
        w_down,
        other_down,
    )
    moe_out = lax.psum_scatter(partial, "tok", scatter_dimension=0, tiled=True)
    mixed = (own_resid.astype(f32) + moe_out.astype(f32)).astype(bf16)
    return (mixed, fresh_key_value)


def solution(mesh):
    in_specs = (
        P(("grp", "tok"), "mdl"),
        P(("grp", "tok"), "mdl", None),
        P(("grp", "tok"), None, "mdl", None, None),
        P(("grp", "tok")),
        P("tok", "mdl", None, None),
        P("mdl", None, "tok"),
        P(),
        P(),
        P(("tok", "mdl"), None, None),
        P(("tok", "mdl"), None, None),
        P(("tok", "mdl"), None, None),
        P(("grp", "tok", "mdl"), None),
        P(("grp", "tok", "mdl"), None),
    )
    out_specs = (P(("grp", "tok", "mdl"), None), P(("grp", "tok"), "mdl", None, None))
    return jax.shard_map(shards, mesh=mesh, in_specs=in_specs, out_specs=out_specs, check_vma=False)
```

```python
import functools
import math

import jax
import jax.numpy as jnp
from jax import lax
from jax.experimental import pallas as pl
from jax.experimental.pallas import tpu as pltpu
from jax.sharding import PartitionSpec as P

EXPERTS = 4
TOPK = 2

eps_norm = 1e-05
rope_base = 1000000.0
mask_fill = -1e30


INTERPRET = False


def shift(x, step):
    size = lax.axis_size("tok")
    return lax.ppermute(x, "tok", [(i, (i + step) % size) for i in range(size)])


def swap(x):
    return lax.ppermute(x, "mdl", [(0, 1), (1, 0)])


def ring_gather(parts):
    size = lax.axis_size("tok")
    here = lax.axis_index("tok")
    yield here, parts
    up, down = list(parts), list(parts)
    for step in range(1, size // 2 + 1):
        up = [shift(p, 1) for p in up]
        last = step == size // 2
        if not last:
            down = [shift(p, -1) for p in down]
        yield (here - step) % size, up
        if not last:
            yield (here + step) % size, down


def ring_scatter_sum(pick):
    size = lax.axis_size("tok")
    here = lax.axis_index("tok")
    half = size // 2

    def joined(arrived, device):
        return [(a.astype(jnp.float32) + b.astype(jnp.float32)) for a, b in zip(arrived, pick(device))]

    up = pick((here + half) % size)
    down = pick((here - half + 1) % size)
    for step in range(1, half + 1):
        up = [shift(p, 1) for p in up]
        if step < half:
            up = [p.astype(jnp.bfloat16) for p in joined(up, (here + half - step) % size)]
            down = [shift(p, -1) for p in down]
            if step < half - 1:
                down = [p.astype(jnp.bfloat16) for p in joined(down, (here - half + 1 + step) % size)]
    own = pick(here)
    return [u.astype(jnp.float32) + d.astype(jnp.float32) + o.astype(jnp.float32) for u, d, o in zip(up, down, own)]


def rms_scale(values_in, gain):
    values = values_in.astype(jnp.float32)
    meansq = jnp.mean(values * values, axis=-1, keepdims=True)
    return values * lax.rsqrt(meansq + eps_norm) * gain.astype(jnp.float32)


def dot(a, b):
    return jnp.dot(a, b, preferred_element_type=jnp.float32)


def score(a, b):
    return lax.dot_general(a, b, (((1,), (1,)), ((), ())), preferred_element_type=jnp.float32)


VMEM = pl.BlockSpec(memory_space=pltpu.VMEM)
SMEM = pl.BlockSpec(memory_space=pltpu.SMEM)
ANY = pl.BlockSpec(memory_space=pl.ANY)


def cache_kernel(scale, length_ref, q_ref, k_ref, v_ref, total_ref, max_ref, sum_ref, s_ref):
    length = length_ref[0]
    block = 512
    steps = k_ref.shape[1] // block
    q = q_ref[0]
    top = None
    for i in range(steps):
        s = score(q, k_ref[0, i * block : (i + 1) * block]) * scale
        column = i * block + lax.broadcasted_iota(jnp.int32, s.shape, 1)
        s = jnp.where(column < length, s, mask_fill)
        s_ref[:, i * block : (i + 1) * block] = s
        high = jnp.max(s, axis=1, keepdims=True)
        top = high if top is None else jnp.maximum(top, high)
    row_sum = jnp.zeros_like(top)
    total = jnp.zeros(total_ref.shape[1:], jnp.float32)
    for i in range(steps):
        s = s_ref[:, i * block : (i + 1) * block]
        column = i * block + lax.broadcasted_iota(jnp.int32, s.shape, 1)
        p = jnp.where(column < length, jnp.exp(s - top), 0.0)
        row_sum += jnp.sum(p, axis=1, keepdims=True)
        total += dot(p.astype(jnp.bfloat16), v_ref[0, i * block : (i + 1) * block])
    total_ref[0] = total
    max_ref[0] = jnp.broadcast_to(top, total.shape)
    sum_ref[0] = jnp.broadcast_to(row_sum, total.shape)


def cache_attention(length, rows, keys, values, scale):
    heads, count, dim = rows.shape
    per_head = lambda n: pl.BlockSpec((1, n, dim), lambda i: (i, 0, 0))
    out = jax.ShapeDtypeStruct((heads, count, dim), jnp.float32)
    return pl.pallas_call(
        functools.partial(cache_kernel, scale),
        grid=(heads,),
        in_specs=[SMEM, per_head(count), per_head(keys.shape[1]), per_head(keys.shape[1])],
        out_specs=[per_head(count)] * 3,
        out_shape=[out] * 3,
        scratch_shapes=[pltpu.VMEM((count, keys.shape[1]), jnp.float32)],
        compiler_params=pltpu.CompilerParams(
            dimension_semantics=("arbitrary",), vmem_limit_bytes=16 * 1024 * 1024
        ),
        cost_estimate=pl.CostEstimate(
            flops=4 * heads * count * dim * keys.shape[1],
            bytes_accessed=4 * keys.size,
            transcendentals=heads * count * keys.shape[1],
        ),
        interpret=INTERPRET,
        name="cache_attention",
    )(length, rows, keys, values)


def fresh_kernel(scale, order, *refs):
    parts = refs[: 2 * len(order)]
    n_ref, cos_ref, sin_ref, q_ref, total_ref, max_ref, sum_ref, heads_ref, fresh_ref, notes_ref = refs[2 * len(order) :]
    half = n_ref.shape[2] // 2
    span = n_ref.shape[1]
    kv = None
    for i, at in enumerate(order):
        more = dot(n_ref[at, :, :half], parts[2 * i][:half]) + dot(n_ref[at, :, half:], parts[2 * i + 1][...])
        kv = more if kv is None else kv + more
        notes_ref[at : at + 1] = parts[2 * i][half:][:1].astype(jnp.float32)
    heads, count, dim = q_ref.shape
    group = count // span
    for h in range(heads):
        k = kv[:, 2 * h * dim : (2 * h + 1) * dim]
        v = kv[:, (2 * h + 1) * dim : (2 * h + 2) * dim].astype(jnp.bfloat16)
        k = (k * cos_ref[...] + pltpu.roll(k, dim // 2, 1) * sin_ref[...]).astype(jnp.bfloat16)
        fresh_ref[:, 2 * h * dim : (2 * h + 1) * dim] = k
        fresh_ref[:, (2 * h + 1) * dim : (2 * h + 2) * dim] = v
        s = score(q_ref[h], k) * scale
        token = lax.broadcasted_iota(jnp.int32, s.shape, 0) % span
        allowed = lax.broadcasted_iota(jnp.int32, s.shape, 1) <= token
        s = jnp.where(allowed, s, mask_fill)
        old_max = max_ref[h][:, :1]
        top = jnp.maximum(old_max, jnp.max(s, axis=1, keepdims=True))
        p = jnp.where(allowed, jnp.exp(s - top), 0.0)
        decay = jnp.exp(old_max - top)
        row_sum = sum_ref[h][:, :1] * decay + jnp.sum(p, axis=1, keepdims=True)
        out = (total_ref[h] * decay + dot(p.astype(jnp.bfloat16), v)) / row_sum
        for g in range(group):
            col = (h * group + g) * dim
            heads_ref[:, col : col + dim] = out[g * span : (g + 1) * span].astype(jnp.bfloat16)


def fresh_attention(parts, order, n_rot, cosine, sine, rows, old, scale):
    span = n_rot.shape[1]
    heads, count, dim = rows.shape
    return pl.pallas_call(
        functools.partial(fresh_kernel, scale, order),
        in_specs=[VMEM] * (len(parts) + 7),
        out_specs=[VMEM, VMEM, VMEM],
        out_shape=[
            jax.ShapeDtypeStruct((span, heads * (count // span) * dim), jnp.bfloat16),
            jax.ShapeDtypeStruct((span, heads * 2 * dim), jnp.bfloat16),
            jax.ShapeDtypeStruct((len(order), heads * 2 * dim), jnp.float32),
        ],
        compiler_params=pltpu.CompilerParams(vmem_limit_bytes=24 * 1024 * 1024),
        interpret=INTERPRET,
        name="fresh_attention",
    )(*parts, n_rot, cosine, sine, rows, *old)


def output_kernel(places_ref, h0, h1, h2, h3a, h3b, c_ref, *refs):
    weights = refs[:8]
    left_ref, right_ref, all_ref = refs[8:]
    n = h0.shape[0]
    all_ref[0:n] = h0[...]
    all_ref[n : 2 * n] = h1[...]
    all_ref[2 * n : 3 * n] = h2[...]
    all_ref[3 * n : 3 * n + n // 2] = h3a[...]
    all_ref[3 * n + n // 2 :] = h3b[...]
    half = all_ref.shape[1] // 2
    mine, other = all_ref[:, :half], all_ref[:, half:]
    block = c_ref.shape[3]
    for j in range(4):
        out = dot(mine, weights[j][...]) + dot(other, weights[4 + j][...])
        target = left_ref if j < 2 else right_ref
        for g in range(4):
            row = pl.multiple_of(places_ref[g] * n, n)
            value = out[g * n : (g + 1) * n] + c_ref[places_ref[g], j].astype(jnp.float32)
            target[pl.ds(row, n), (j % 2) * block : (j % 2 + 1) * block] = value.astype(jnp.bfloat16)


def output_rows(places, heads, cols, weights):
    n, width = heads[0].shape
    block = cols.shape[3]
    out = jax.ShapeDtypeStruct((4 * n, 2 * block), jnp.bfloat16)
    return pl.pallas_call(
        output_kernel,
        in_specs=[SMEM] + [VMEM] * 14,
        out_specs=[VMEM, VMEM],
        out_shape=[out, out],
        scratch_shapes=[pltpu.VMEM((4 * n, width), jnp.bfloat16)],
        compiler_params=pltpu.CompilerParams(vmem_limit_bytes=24 * 1024 * 1024),
        interpret=INTERPRET,
        name="output_rows",
    )(places, *heads, cols, *weights)


def expert_kernel(sources, k_steps, ahead, src_ref, *refs):
    parts = refs[: 2 * sources]
    (pick_ref, spread_ref, weight_ref, gain_ref, g0, u0, g1, u1, d0, d1, out_ref, own_ref,
     x, wbuf, dbuf, wsem, xsem, xs, ga, ua, hid) = refs[2 * sources :]
    model = x.shape[1]
    ff = ga.shape[1]
    width = model // k_steps
    group = parts[0].shape[0]
    block = parts[0].shape[1] // 2
    total = 3 * k_steps

    def copies(step):
        phase, k = divmod(step, k_steps)
        slot = step % ahead if phase < 2 else k
        if phase < 2:
            pair, target = ((g0, u0), (g1, u1))[phase], wbuf
            window = lambda w: w.at[0, pl.ds(k * width, width), :]
        else:
            pair, target = (d0, d1), dbuf
            window = lambda w: w.at[0, :, pl.ds(k * width, width)]
        return [
            pltpu.make_async_copy(window(w), target.at[slot, i], wsem.at[step, i])
            for i, w in enumerate(pair)
        ]

    def piece_copies():
        for i in range(sources):
            s = src_ref[i]
            row = pl.multiple_of((s % 4) * group, group)
            for j in range(4):
                col = pl.multiple_of(((s + (sources - 1 + j)) % sources) * block, block)
                yield pltpu.make_async_copy(
                    parts[2 * i + j // 2].at[:, pl.ds((j % 2) * block, block)],
                    x.at[pl.ds(row, group), pl.ds(col, block)],
                    xsem.at[i, j],
                )

    for c in piece_copies():
        c.start()
    for step in range(ahead):
        for c in copies(step):
            c.start()
    for c in piece_copies():
        c.wait()
    here = src_ref[0]
    own_row = (here % 4) * group + (here // 4) * (group // 4)
    own_ref[...] = x[pl.ds(pl.multiple_of(own_row, group // 4), group // 4), :]

    squares = None
    for k in range(k_steps):
        cols = slice(k * width, (k + 1) * width)
        rows = dot(pick_ref[...], x[:, cols])
        more = jnp.sum(rows * rows, axis=1, keepdims=True)
        squares = more if squares is None else squares + more
        xs[:, cols] = (rows * gain_ref[:, cols]).astype(jnp.bfloat16)
    scale = lax.rsqrt(squares * (1.0 / model) + eps_norm)

    for step in range(total):
        phase, k = divmod(step, k_steps)
        slot = step % ahead if phase < 2 else k
        for c in copies(step):
            c.wait()
        if phase < 2:
            tile = xs[:, k * width : (k + 1) * width]
            g, u = dot(tile, wbuf[slot, 0]), dot(tile, wbuf[slot, 1])
            if k == 0:
                ga[...] = g
                ua[...] = u
            elif k < k_steps - 1:
                ga[...] += g
                ua[...] += u
            else:
                gv, uv = (ga[...] + g) * scale, (ua[...] + u) * scale
                hid[:, phase * ff : (phase + 1) * ff] = (gv / (1.0 + jnp.exp(-gv)) * uv).astype(jnp.bfloat16)
        else:
            rows = dot(hid[:, :ff], dbuf[slot, 0]) + dot(hid[:, ff:], dbuf[slot, 1])
        if step + ahead < total:
            for c in copies(step + ahead):
                c.start()
        if phase == 2:
            out = dot(spread_ref[...], rows.astype(jnp.bfloat16)) * weight_ref[...]
            out_ref[:, k * width : (k + 1) * width] = out.astype(jnp.bfloat16)


def expert_rows(sources, parts, pick, spread, weight, gain, gates0, ups0, gates1, ups1, downs0, downs1):
    rows, tokens = pick.shape
    ff, model = downs0.shape[1:]
    k_steps, ahead = 4, 3
    width = model // k_steps
    count = sources.shape[0]
    return pl.pallas_call(
        functools.partial(expert_kernel, count, k_steps, ahead),
        in_specs=[SMEM] + [ANY] * len(parts) + [VMEM] * 4 + [ANY] * 6,
        out_specs=[VMEM, VMEM],
        out_shape=[
            jax.ShapeDtypeStruct((tokens, model), jnp.bfloat16),
            jax.ShapeDtypeStruct((tokens // count, model), jnp.bfloat16),
        ],
        scratch_shapes=[
            pltpu.VMEM((tokens, model), jnp.bfloat16),
            pltpu.VMEM((ahead, 2, width, ff), jnp.bfloat16),
            pltpu.VMEM((k_steps, 2, ff, width), jnp.bfloat16),
            pltpu.SemaphoreType.DMA((3 * k_steps, 2)),
            pltpu.SemaphoreType.DMA((count, 4)),
            pltpu.VMEM((rows, model), jnp.bfloat16),
            pltpu.VMEM((rows, ff), jnp.float32),
            pltpu.VMEM((rows, ff), jnp.float32),
            pltpu.VMEM((rows, 2 * ff), jnp.bfloat16),
        ],
        compiler_params=pltpu.CompilerParams(vmem_limit_bytes=46 * 1024 * 1024),
        cost_estimate=pl.CostEstimate(
            flops=12 * rows * model * ff, bytes_accessed=12 * model * ff, transcendentals=2 * rows * ff
        ),
        interpret=INTERPRET,
        name="experts",
    )(sources, *parts, pick, spread, weight, gain, gates0, ups0, gates1, ups1, downs0, downs1)


def rotated(blocks, here):
    return lax.dynamic_slice_in_dim(jnp.concatenate([blocks, blocks], axis=0), here, blocks.shape[0], 0)


def shards(
    hidden,
    queries,
    cache,
    cache_lengths,
    wkv,
    wo,
    attn_gain,
    moe_gain,
    w_gate,
    w_up,
    w_down,
    expert_ids,
    gates,
):
    size = lax.axis_size("tok")
    here = lax.axis_index("tok")
    core = lax.axis_index("mdl")
    cores = lax.axis_size("mdl")
    bf16, f32 = jnp.bfloat16, jnp.float32

    matches = expert_ids[:, :, None] == jnp.arange(EXPERTS)[None, None, :]
    route = jnp.sum(jnp.where(matches, gates[:, :, None], 0.0), axis=1).T
    coarse = lax.reduce_precision(route, 8, 7)
    note = jnp.concatenate([coarse, route - coarse], axis=0).astype(bf16).reshape(1, -1)
    kv_heads, head_dim = wkv.shape[1], wkv.shape[3]
    own_kv = wkv.reshape(wkv.shape[0], -1)
    half = own_kv.shape[0] // 2
    note = jnp.pad(note, ((0, 7), (0, own_kv.shape[1] - note.shape[1])))
    kv_parts, order = [], []
    for i, (source, pair) in enumerate(ring_gather([jnp.concatenate([own_kv[:half], note], axis=0), own_kv[half:]])):
        kv_parts += pair
        order.append((-((i + 1) // 2) if i % 2 else i // 2) % size)

    other_hidden = swap(hidden)
    low = jnp.where(core == 0, hidden, other_hidden)
    high = jnp.where(core == 0, other_hidden, hidden)
    full_rows = jnp.concatenate([low, high], axis=1)
    span_len, model = full_rows.shape
    core_rows = span_len // cores
    block = model // size
    normed = rms_scale(full_rows, attn_gain).astype(bf16)
    n_rot = rotated(jnp.moveaxis(normed.reshape(span_len, size, block), 1, 0), here)

    own_rows = lax.dynamic_slice_in_dim(full_rows, core * core_rows, core_rows, 0)
    blocks = jnp.moveaxis(own_rows.reshape(core_rows, size, block), 1, 0)
    blocks = rotated(blocks, (here + size - 1) % 4 + jnp.where(here % 4 == 0, size - 4, 0))
    cols = lax.all_to_all(
        blocks.reshape(size // 4, 4, core_rows, block),
        "tok",
        0,
        0,
        axis_index_groups=[list(range(b, size, 4)) for b in range(4)],
        tiled=True,
    )

    own_wo = wo.reshape(-1, wo.shape[2])
    next_wo = shift(own_wo, -1)
    mine_wo = [shift(own_wo, 1), own_wo, next_wo, shift(next_wo, -1)]
    full_wo = mine_wo + [swap(w) for w in mine_wo]

    other_gate, other_up, other_down = swap(w_gate), swap(w_up), swap(w_down)

    length = cache_lengths[0]
    head_group = queries.shape[1] // kv_heads
    scale_factor = 1.0 / math.sqrt(head_dim)
    rows = jnp.swapaxes(queries, 0, 1).reshape(kv_heads, head_group * span_len, head_dim)
    keys = jnp.stack([cache[0, :, h, 0] for h in range(kv_heads)])
    values = jnp.stack([cache[0, :, h, 1] for h in range(kv_heads)])
    old = cache_attention(cache_lengths, rows, keys, values, scale_factor)

    positions = (length + jnp.arange(span_len, dtype=jnp.int32)).astype(f32)
    inverse = jnp.exp(
        jnp.arange(head_dim // 2, dtype=f32) * (-2.0 * math.log(rope_base) / head_dim)
    )
    angle = positions[:, None] * inverse[None, :]
    cosine, sine = jnp.cos(angle), jnp.sin(angle)
    heads_out, fresh, notes = fresh_attention(
        kv_parts,
        order,
        n_rot,
        jnp.concatenate([cosine, cosine], axis=1),
        jnp.concatenate([-sine, sine], axis=1),
        rows,
        old,
        scale_factor,
    )
    fresh_key_value = fresh.reshape(span_len, kv_heads, 2, head_dim)

    notes = notes[:, : 2 * EXPERTS * core_rows].reshape(size, 2, EXPERTS, core_rows)
    weight = lax.dynamic_index_in_dim(notes[:, 0] + notes[:, 1], here * EXPERTS // size, 1, keepdims=False)
    weight = rotated(weight, (size - here) % size)
    weight = jnp.swapaxes(weight.reshape(size // 4, 4, core_rows), 0, 1).reshape(size, core_rows)
    chosen = (weight > 0).astype(jnp.int32)
    rank = jnp.cumsum(chosen, axis=1) - chosen
    capacity = core_rows * TOPK * 9 // (8 * EXPERTS)
    slot = jnp.where(chosen > 0, rank + jnp.arange(size)[:, None] * capacity, -1).reshape(1, -1)
    pick = (jnp.arange(size * capacity)[:, None] == slot).astype(bf16)
    spread = (slot.reshape(-1, 1) == jnp.arange(size * capacity)[None, :]).astype(bf16)


    kept = lax.dynamic_slice_in_dim(heads_out, core * core_rows, core_rows, 0)
    given = lax.dynamic_slice_in_dim(heads_out, (cores - 1 - core) * core_rows, core_rows, 0)
    own_heads = jnp.concatenate([kept, swap(given)], axis=1)
    back, ahead = shift(own_heads, 4), shift(own_heads, -4)
    far = [shift(back[: core_rows // 2], 4), shift(ahead[core_rows // 2 :], -4)]
    places = (here // 4 + jnp.array([0, 3, 1, 2], jnp.int32)) % 4
    left, right = output_rows(places, [own_heads, back, ahead, *far], cols, full_wo)

    parts, sources = [], []
    for source, pair in ring_gather([left, right]):
        parts += pair
        sources.append(source)

    partial, own_resid = expert_rows(
        jnp.stack(sources).astype(jnp.int32),
        parts,
        pick,
        spread,
        weight.reshape(-1, 1),
        moe_gain.astype(f32).reshape(1, -1),
        w_gate,
        w_up,
        other_gate,
        other_up,
        w_down,
        other_down,
    )
    partial = partial.reshape(size, core_rows, model)

    def pieces(device):
        at = (device % 4) * (size // 4) + device // 4
        mine = lax.dynamic_index_in_dim(partial, at, 0, keepdims=False)
        return [mine[:, : model // 2], mine[:, model // 2 :]]

    moe_out = jnp.concatenate(ring_scatter_sum(pieces), axis=1)
    mixed = (own_resid.astype(f32) + moe_out).astype(bf16)
    return (mixed, fresh_key_value)


def solution(mesh):
    in_specs = (
        P(("grp", "tok"), "mdl"),
        P(("grp", "tok"), "mdl", None),
        P(("grp", "tok"), None, "mdl", None, None),
        P(("grp", "tok")),
        P("tok", "mdl", None, None),
        P("mdl", None, "tok"),
        P(),
        P(),
        P(("tok", "mdl"), None, None),
        P(("tok", "mdl"), None, None),
        P(("tok", "mdl"), None, None),
        P(("grp", "tok", "mdl"), None),
        P(("grp", "tok", "mdl"), None),
    )
    out_specs = (P(("grp", "tok", "mdl"), None), P(("grp", "tok"), "mdl", None, None))
    return jax.shard_map(shards, mesh=mesh, in_specs=in_specs, out_specs=out_specs, check_vma=False)
```

```python
import functools
import math

import jax
import jax.numpy as jnp
from jax import lax
from jax.experimental import pallas as pl
from jax.experimental.pallas import tpu as pltpu
from jax.sharding import PartitionSpec as P

EXPERTS = 4
TOPK = 2

eps_norm = 1e-05
rope_base = 1000000.0
mask_fill = -1e30


INTERPRET = False


def shift(x, step):
    size = lax.axis_size("tok")
    return lax.ppermute(x, "tok", [(i, (i + step) % size) for i in range(size)])


def swap(x):
    return lax.ppermute(x, "mdl", [(0, 1), (1, 0)])


def ring_gather(parts):
    size = lax.axis_size("tok")
    here = lax.axis_index("tok")
    yield here, parts
    up, down = list(parts), list(parts)
    for step in range(1, size // 2 + 1):
        up = [shift(p, 1) for p in up]
        last = step == size // 2
        if not last:
            down = [shift(p, -1) for p in down]
        yield (here - step) % size, up
        if not last:
            yield (here + step) % size, down


def ring_scatter_sum(pick):
    size = lax.axis_size("tok")
    here = lax.axis_index("tok")
    half = size // 2

    def joined(arrived, device):
        return [(a.astype(jnp.float32) + b.astype(jnp.float32)) for a, b in zip(arrived, pick(device))]

    up = pick((here + half) % size)
    down = pick((here - half + 1) % size)
    for step in range(1, half + 1):
        up = [shift(p, 1) for p in up]
        if step < half:
            up = [p.astype(jnp.bfloat16) for p in joined(up, (here + half - step) % size)]
            down = [shift(p, -1) for p in down]
            if step < half - 1:
                down = [p.astype(jnp.bfloat16) for p in joined(down, (here - half + 1 + step) % size)]
    own = pick(here)
    return [u.astype(jnp.float32) + d.astype(jnp.float32) + o.astype(jnp.float32) for u, d, o in zip(up, down, own)]


def rms_scale(values_in, gain):
    values = values_in.astype(jnp.float32)
    meansq = jnp.mean(values * values, axis=-1, keepdims=True)
    return values * lax.rsqrt(meansq + eps_norm) * gain.astype(jnp.float32)


def dot(a, b):
    return jnp.dot(a, b, preferred_element_type=jnp.float32)


def score(a, b):
    return lax.dot_general(a, b, (((1,), (1,)), ((), ())), preferred_element_type=jnp.float32)


VMEM = pl.BlockSpec(memory_space=pltpu.VMEM)
SMEM = pl.BlockSpec(memory_space=pltpu.SMEM)
ANY = pl.BlockSpec(memory_space=pl.ANY)


def cache_kernel(scale, length_ref, q_ref, k_ref, v_ref, total_ref, max_ref, sum_ref, s_ref):
    length = length_ref[0]
    block = 512
    steps = k_ref.shape[1] // block
    q = q_ref[0]
    top = None
    for i in range(steps):
        s = score(q, k_ref[0, i * block : (i + 1) * block]) * scale
        column = i * block + lax.broadcasted_iota(jnp.int32, s.shape, 1)
        s = jnp.where(column < length, s, mask_fill)
        s_ref[:, i * block : (i + 1) * block] = s
        high = jnp.max(s, axis=1, keepdims=True)
        top = high if top is None else jnp.maximum(top, high)
    row_sum = jnp.zeros_like(top)
    total = jnp.zeros(total_ref.shape[1:], jnp.float32)
    for i in range(steps):
        s = s_ref[:, i * block : (i + 1) * block]
        column = i * block + lax.broadcasted_iota(jnp.int32, s.shape, 1)
        p = jnp.where(column < length, jnp.exp(s - top), 0.0)
        row_sum += jnp.sum(p, axis=1, keepdims=True)
        total += dot(p.astype(jnp.bfloat16), v_ref[0, i * block : (i + 1) * block])
    total_ref[0] = total
    max_ref[0] = jnp.broadcast_to(top, total.shape)
    sum_ref[0] = jnp.broadcast_to(row_sum, total.shape)


def cache_attention(length, rows, keys, values, scale):
    heads, count, dim = rows.shape
    per_head = lambda n: pl.BlockSpec((1, n, dim), lambda i: (i, 0, 0))
    out = jax.ShapeDtypeStruct((heads, count, dim), jnp.float32)
    return pl.pallas_call(
        functools.partial(cache_kernel, scale),
        grid=(heads,),
        in_specs=[SMEM, per_head(count), per_head(keys.shape[1]), per_head(keys.shape[1])],
        out_specs=[per_head(count)] * 3,
        out_shape=[out] * 3,
        scratch_shapes=[pltpu.VMEM((count, keys.shape[1]), jnp.float32)],
        compiler_params=pltpu.CompilerParams(
            dimension_semantics=("arbitrary",), vmem_limit_bytes=16 * 1024 * 1024
        ),
        cost_estimate=pl.CostEstimate(
            flops=4 * heads * count * dim * keys.shape[1],
            bytes_accessed=4 * keys.size,
            transcendentals=heads * count * keys.shape[1],
        ),
        interpret=INTERPRET,
        name="cache_attention",
    )(length, rows, keys, values)


def fresh_kernel(scale, order, *refs):
    parts = refs[: 2 * len(order)]
    n_ref, cos_ref, sin_ref, q_ref, total_ref, max_ref, sum_ref, heads_ref, fresh_ref, notes_ref = refs[2 * len(order) :]
    half = n_ref.shape[2] // 2
    span = n_ref.shape[1]
    kv = None
    for i, at in enumerate(order):
        more = dot(n_ref[at, :, :half], parts[2 * i][:half]) + dot(n_ref[at, :, half:], parts[2 * i + 1][...])
        kv = more if kv is None else kv + more
        notes_ref[at : at + 1] = parts[2 * i][half:][:1].astype(jnp.float32)
    heads, count, dim = q_ref.shape
    group = count // span
    for h in range(heads):
        k = kv[:, 2 * h * dim : (2 * h + 1) * dim]
        v = kv[:, (2 * h + 1) * dim : (2 * h + 2) * dim].astype(jnp.bfloat16)
        k = (k * cos_ref[...] + pltpu.roll(k, dim // 2, 1) * sin_ref[...]).astype(jnp.bfloat16)
        fresh_ref[:, 2 * h * dim : (2 * h + 1) * dim] = k
        fresh_ref[:, (2 * h + 1) * dim : (2 * h + 2) * dim] = v
        s = score(q_ref[h], k) * scale
        token = lax.broadcasted_iota(jnp.int32, s.shape, 0) % span
        allowed = lax.broadcasted_iota(jnp.int32, s.shape, 1) <= token
        s = jnp.where(allowed, s, mask_fill)
        old_max = max_ref[h][:, :1]
        top = jnp.maximum(old_max, jnp.max(s, axis=1, keepdims=True))
        p = jnp.where(allowed, jnp.exp(s - top), 0.0)
        decay = jnp.exp(old_max - top)
        row_sum = sum_ref[h][:, :1] * decay + jnp.sum(p, axis=1, keepdims=True)
        out = (total_ref[h] * decay + dot(p.astype(jnp.bfloat16), v)) / row_sum
        for g in range(group):
            col = (h * group + g) * dim
            heads_ref[:, col : col + dim] = out[g * span : (g + 1) * span].astype(jnp.bfloat16)


def fresh_attention(parts, order, n_rot, cosine, sine, rows, old, scale):
    span = n_rot.shape[1]
    heads, count, dim = rows.shape
    return pl.pallas_call(
        functools.partial(fresh_kernel, scale, order),
        in_specs=[VMEM] * (len(parts) + 7),
        out_specs=[VMEM, VMEM, VMEM],
        out_shape=[
            jax.ShapeDtypeStruct((span, heads * (count // span) * dim), jnp.bfloat16),
            jax.ShapeDtypeStruct((span, heads * 2 * dim), jnp.bfloat16),
            jax.ShapeDtypeStruct((len(order), heads * 2 * dim), jnp.float32),
        ],
        compiler_params=pltpu.CompilerParams(vmem_limit_bytes=24 * 1024 * 1024),
        interpret=INTERPRET,
        name="fresh_attention",
    )(*parts, n_rot, cosine, sine, rows, *old)


def output_kernel(places_ref, h0, h1, h2, h3a, h3b, c0, c1, c2, c3, *refs):
    weights = refs[:8]
    left_ref, right_ref, all_ref = refs[8:]
    n = h0.shape[0]
    all_ref[0:n] = h0[...]
    all_ref[n : 2 * n] = h1[...]
    all_ref[2 * n : 3 * n] = h2[...]
    all_ref[3 * n : 3 * n + n // 2] = h3a[...]
    all_ref[3 * n + n // 2 :] = h3b[...]
    half = all_ref.shape[1] // 2
    mine, other = all_ref[:, :half], all_ref[:, half:]
    block = c0.shape[2]
    for j in range(4):
        out = dot(mine, weights[j][...]) + dot(other, weights[4 + j][...])
        target = left_ref if j < 2 else right_ref
        for g, c in enumerate((c0, c1, c2, c3)):
            row = pl.multiple_of(places_ref[g] * n, n)
            value = out[g * n : (g + 1) * n] + c[j].astype(jnp.float32)
            target[pl.ds(row, n), (j % 2) * block : (j % 2 + 1) * block] = value.astype(jnp.bfloat16)


def output_rows(places, heads, cols, weights):
    n, width = heads[0].shape
    block = cols[0].shape[2]
    out = jax.ShapeDtypeStruct((4 * n, 2 * block), jnp.bfloat16)
    return pl.pallas_call(
        output_kernel,
        in_specs=[SMEM] + [VMEM] * 17,
        out_specs=[VMEM, VMEM],
        out_shape=[out, out],
        scratch_shapes=[pltpu.VMEM((4 * n, width), jnp.bfloat16)],
        compiler_params=pltpu.CompilerParams(vmem_limit_bytes=24 * 1024 * 1024),
        interpret=INTERPRET,
        name="output_rows",
    )(places, *heads, *cols, *weights)


def expert_kernel(sources, k_steps, ahead, src_ref, *refs):
    parts = refs[: 2 * sources]
    (pick_ref, spread_ref, weight_ref, gain_ref, g0, u0, g1, u1, d0, d1, out_ref, own_ref,
     x, wbuf, dbuf, wsem, xsem, xs, ga, ua, hid) = refs[2 * sources :]
    model = x.shape[1]
    ff = ga.shape[1]
    width = model // k_steps
    group = parts[0].shape[0]
    block = parts[0].shape[1] // 2
    total = 3 * k_steps

    def copies(step):
        phase, k = divmod(step, k_steps)
        slot = step % ahead if phase < 2 else k
        if phase < 2:
            pair, target = ((g0, u0), (g1, u1))[phase], wbuf
            window = lambda w: w.at[0, pl.ds(k * width, width), :]
        else:
            pair, target = (d0, d1), dbuf
            window = lambda w: w.at[0, :, pl.ds(k * width, width)]
        return [
            pltpu.make_async_copy(window(w), target.at[slot, i], wsem.at[step, i])
            for i, w in enumerate(pair)
        ]

    def piece_copies():
        for i in range(sources):
            s = src_ref[i]
            row = pl.multiple_of((s % 4) * group, group)
            for j in range(4):
                col = pl.multiple_of(((s + (sources - 1 + j)) % sources) * block, block)
                yield pltpu.make_async_copy(
                    parts[2 * i + j // 2].at[:, pl.ds((j % 2) * block, block)],
                    x.at[pl.ds(row, group), pl.ds(col, block)],
                    xsem.at[i, j],
                )

    for c in piece_copies():
        c.start()
    for step in range(ahead):
        for c in copies(step):
            c.start()
    for c in piece_copies():
        c.wait()
    here = src_ref[0]
    own_row = (here % 4) * group + (here // 4) * (group // 4)
    own_ref[...] = x[pl.ds(pl.multiple_of(own_row, group // 4), group // 4), :]

    squares = None
    for k in range(k_steps):
        cols = slice(k * width, (k + 1) * width)
        rows = dot(pick_ref[...], x[:, cols])
        more = jnp.sum(rows * rows, axis=1, keepdims=True)
        squares = more if squares is None else squares + more
        xs[:, cols] = (rows * gain_ref[:, cols]).astype(jnp.bfloat16)
    scale = lax.rsqrt(squares * (1.0 / model) + eps_norm)

    for step in range(total):
        phase, k = divmod(step, k_steps)
        slot = step % ahead if phase < 2 else k
        for c in copies(step):
            c.wait()
        if phase < 2:
            tile = xs[:, k * width : (k + 1) * width]
            g, u = dot(tile, wbuf[slot, 0]), dot(tile, wbuf[slot, 1])
            if k == 0:
                ga[...] = g
                ua[...] = u
            elif k < k_steps - 1:
                ga[...] += g
                ua[...] += u
            else:
                gv, uv = (ga[...] + g) * scale, (ua[...] + u) * scale
                hid[:, phase * ff : (phase + 1) * ff] = (gv / (1.0 + jnp.exp(-gv)) * uv).astype(jnp.bfloat16)
        else:
            rows = dot(hid[:, :ff], dbuf[slot, 0]) + dot(hid[:, ff:], dbuf[slot, 1])
        if step + ahead < total:
            for c in copies(step + ahead):
                c.start()
        if phase == 2:
            out = dot(spread_ref[...], rows.astype(jnp.bfloat16)) * weight_ref[...]
            out_ref[:, k * width : (k + 1) * width] = out.astype(jnp.bfloat16)


def expert_rows(sources, parts, pick, spread, weight, gain, gates0, ups0, gates1, ups1, downs0, downs1):
    rows, tokens = pick.shape
    ff, model = downs0.shape[1:]
    k_steps, ahead = 4, 3
    width = model // k_steps
    count = sources.shape[0]
    return pl.pallas_call(
        functools.partial(expert_kernel, count, k_steps, ahead),
        in_specs=[SMEM] + [ANY] * len(parts) + [VMEM] * 4 + [ANY] * 6,
        out_specs=[VMEM, VMEM],
        out_shape=[
            jax.ShapeDtypeStruct((tokens, model), jnp.bfloat16),
            jax.ShapeDtypeStruct((tokens // count, model), jnp.bfloat16),
        ],
        scratch_shapes=[
            pltpu.VMEM((tokens, model), jnp.bfloat16),
            pltpu.VMEM((ahead, 2, width, ff), jnp.bfloat16),
            pltpu.VMEM((k_steps, 2, ff, width), jnp.bfloat16),
            pltpu.SemaphoreType.DMA((3 * k_steps, 2)),
            pltpu.SemaphoreType.DMA((count, 4)),
            pltpu.VMEM((rows, model), jnp.bfloat16),
            pltpu.VMEM((rows, ff), jnp.float32),
            pltpu.VMEM((rows, ff), jnp.float32),
            pltpu.VMEM((rows, 2 * ff), jnp.bfloat16),
        ],
        compiler_params=pltpu.CompilerParams(vmem_limit_bytes=46 * 1024 * 1024),
        cost_estimate=pl.CostEstimate(
            flops=12 * rows * model * ff, bytes_accessed=12 * model * ff, transcendentals=2 * rows * ff
        ),
        interpret=INTERPRET,
        name="experts",
    )(sources, *parts, pick, spread, weight, gain, gates0, ups0, gates1, ups1, downs0, downs1)


def rotated(blocks, here):
    return lax.dynamic_slice_in_dim(jnp.concatenate([blocks, blocks], axis=0), here, blocks.shape[0], 0)


def shards(
    hidden,
    queries,
    cache,
    cache_lengths,
    wkv,
    wo,
    attn_gain,
    moe_gain,
    w_gate,
    w_up,
    w_down,
    expert_ids,
    gates,
):
    size = lax.axis_size("tok")
    here = lax.axis_index("tok")
    core = lax.axis_index("mdl")
    cores = lax.axis_size("mdl")
    bf16, f32 = jnp.bfloat16, jnp.float32

    matches = expert_ids[:, :, None] == jnp.arange(EXPERTS)[None, None, :]
    route = jnp.sum(jnp.where(matches, gates[:, :, None], 0.0), axis=1).T
    coarse = lax.reduce_precision(route, 8, 7)
    note = jnp.concatenate([coarse, route - coarse], axis=0).astype(bf16).reshape(1, -1)
    kv_heads, head_dim = wkv.shape[1], wkv.shape[3]
    own_kv = wkv.reshape(wkv.shape[0], -1)
    half = own_kv.shape[0] // 2
    note = jnp.pad(note, ((0, 7), (0, own_kv.shape[1] - note.shape[1])))
    kv_parts, order = [], []
    for i, (source, pair) in enumerate(ring_gather([jnp.concatenate([own_kv[:half], note], axis=0), own_kv[half:]])):
        kv_parts += pair
        order.append((-((i + 1) // 2) if i % 2 else i // 2) % size)

    other_hidden = swap(hidden)
    low = jnp.where(core == 0, hidden, other_hidden)
    high = jnp.where(core == 0, other_hidden, hidden)
    full_rows = jnp.concatenate([low, high], axis=1)
    span_len, model = full_rows.shape
    core_rows = span_len // cores
    block = model // size
    normed = rms_scale(full_rows, attn_gain).astype(bf16)
    n_rot = rotated(jnp.moveaxis(normed.reshape(span_len, size, block), 1, 0), here)

    own_rows = lax.dynamic_slice_in_dim(full_rows, core * core_rows, core_rows, 0)
    h_rot = rotated(jnp.moveaxis(own_rows.reshape(core_rows, size, block), 1, 0), here)
    cols = [
        jnp.concatenate([h_rot[size - 1 :], h_rot[:3]], axis=0),
        shift(h_rot[3:7], 4),
        shift(h_rot[size - 5 : size - 1], -4),
        shift(h_rot[7:11], 8),
    ]

    own_wo = wo.reshape(-1, wo.shape[2])
    next_wo = shift(own_wo, -1)
    mine_wo = [shift(own_wo, 1), own_wo, next_wo, shift(next_wo, -1)]
    full_wo = mine_wo + [swap(w) for w in mine_wo]

    other_gate, other_up, other_down = swap(w_gate), swap(w_up), swap(w_down)

    length = cache_lengths[0]
    head_group = queries.shape[1] // kv_heads
    scale_factor = 1.0 / math.sqrt(head_dim)
    rows = jnp.swapaxes(queries, 0, 1).reshape(kv_heads, head_group * span_len, head_dim)
    keys = jnp.stack([cache[0, :, h, 0] for h in range(kv_heads)])
    values = jnp.stack([cache[0, :, h, 1] for h in range(kv_heads)])
    old = cache_attention(cache_lengths, rows, keys, values, scale_factor)

    positions = (length + jnp.arange(span_len, dtype=jnp.int32)).astype(f32)
    inverse = jnp.exp(
        jnp.arange(head_dim // 2, dtype=f32) * (-2.0 * math.log(rope_base) / head_dim)
    )
    angle = positions[:, None] * inverse[None, :]
    cosine, sine = jnp.cos(angle), jnp.sin(angle)
    heads_out, fresh, notes = fresh_attention(
        kv_parts,
        order,
        n_rot,
        jnp.concatenate([cosine, cosine], axis=1),
        jnp.concatenate([-sine, sine], axis=1),
        rows,
        old,
        scale_factor,
    )
    fresh_key_value = fresh.reshape(span_len, kv_heads, 2, head_dim)

    notes = notes[:, : 2 * EXPERTS * core_rows].reshape(size, 2, EXPERTS, core_rows)
    weight = lax.dynamic_index_in_dim(notes[:, 0] + notes[:, 1], here * EXPERTS // size, 1, keepdims=False)
    weight = rotated(weight, (size - here) % size)
    weight = jnp.swapaxes(weight.reshape(size // 4, 4, core_rows), 0, 1).reshape(size, core_rows)
    chosen = (weight > 0).astype(jnp.int32)
    rank = jnp.cumsum(chosen, axis=1) - chosen
    capacity = core_rows * TOPK * 9 // (8 * EXPERTS)
    slot = jnp.where(chosen > 0, rank + jnp.arange(size)[:, None] * capacity, -1).reshape(1, -1)
    pick = (jnp.arange(size * capacity)[:, None] == slot).astype(bf16)
    spread = (slot.reshape(-1, 1) == jnp.arange(size * capacity)[None, :]).astype(bf16)


    kept = lax.dynamic_slice_in_dim(heads_out, core * core_rows, core_rows, 0)
    given = lax.dynamic_slice_in_dim(heads_out, (cores - 1 - core) * core_rows, core_rows, 0)
    own_heads = jnp.concatenate([kept, swap(given)], axis=1)
    back, ahead = shift(own_heads, 4), shift(own_heads, -4)
    far = [shift(back[: core_rows // 2], 4), shift(ahead[core_rows // 2 :], -4)]
    places = (here // 4 + jnp.array([0, 3, 1, 2], jnp.int32)) % 4
    left, right = output_rows(places, [own_heads, back, ahead, *far], cols, full_wo)

    parts, sources = [], []
    for source, pair in ring_gather([left, right]):
        parts += pair
        sources.append(source)

    partial, own_resid = expert_rows(
        jnp.stack(sources).astype(jnp.int32),
        parts,
        pick,
        spread,
        weight.reshape(-1, 1),
        moe_gain.astype(f32).reshape(1, -1),
        w_gate,
        w_up,
        other_gate,
        other_up,
        w_down,
        other_down,
    )
    partial = partial.reshape(size, core_rows, model)

    def pieces(device):
        at = (device % 4) * (size // 4) + device // 4
        mine = lax.dynamic_index_in_dim(partial, at, 0, keepdims=False)
        return [mine[:, : model // 2], mine[:, model // 2 :]]

    moe_out = jnp.concatenate(ring_scatter_sum(pieces), axis=1)
    mixed = (own_resid.astype(f32) + moe_out).astype(bf16)
    return (mixed, fresh_key_value)


def solution(mesh):
    in_specs = (
        P(("grp", "tok"), "mdl"),
        P(("grp", "tok"), "mdl", None),
        P(("grp", "tok"), None, "mdl", None, None),
        P(("grp", "tok")),
        P("tok", "mdl", None, None),
        P("mdl", None, "tok"),
        P(),
        P(),
        P(("tok", "mdl"), None, None),
        P(("tok", "mdl"), None, None),
        P(("tok", "mdl"), None, None),
        P(("grp", "tok", "mdl"), None),
        P(("grp", "tok", "mdl"), None),
    )
    out_specs = (P(("grp", "tok", "mdl"), None), P(("grp", "tok"), "mdl", None, None))
    return jax.shard_map(shards, mesh=mesh, in_specs=in_specs, out_specs=out_specs, check_vma=False)
```
